32 devices in a mesh: south: 4 (over y, x), east: 4 (over z), down: 2 (over core).
Axes of the slice: x: 2, y: 2, z: 4, core: 2. Of those that a mesh axis runs over, the one named last changes fastest.
Arguments:
- field_values: float32 [32, 384, 16, 128], P('south', 'east', 'down'), may hold values from 0.2 to 1.8
- flow_y: float32 [32, 384, 16, 128], P('south', 'east', 'down'), may hold values from -0.3 to 0.3
- flow_x: float32 [32, 384, 16, 128], P('south', 'east', 'down'), may hold values from -0.3 to 0.3
- flow_z: float32 [32, 384, 16, 128], P('south', 'east', 'down'), may hold values from -0.3 to 0.3
Outputs:
- potential: float32 [32, 384, 16, 128], P('south', 'east', 'down')
- field_values_end: float32 [32, 384, 16, 128], P('south', 'east', 'down')
The draws below stay inside these ranges and needn't reach their ends.
All inputs are finite; a program needn't handle non-finite values.
Results may differ from the reference program's by a relative error of at most 0.00002.
Values sent between devices are 32-bit elements; how exact they have to be, the bound alone decides.
A program may use at most 128 MiB of HBM per device.

```python
import jax
import jax.numpy as jnp
from jax import lax

GRID_Y = 32
GRID_X = 384
GRID_Z = 16
LEVELS = 128
STEPS = 4


def level_of(own_key, extent, cuts, low, largest):
    factor_of = 1.0
    for position, parts in cuts:
        steps = jax.random.uniform(jax.random.fold_in(jax.random.fold_in(own_key, 6), position), (parts,), jnp.float32, low / len(cuts), largest / len(cuts))
        factor_of = factor_of * jnp.repeat(jnp.exp(steps), extent[position] // parts).reshape((-1,) + (1,) * (len(extent) - 1 - position))
    return factor_of


def setup_inputs(seed: int = 0) -> dict:
    seeds = jax.random.split(jax.random.key(seed), 5)
    field_values = jnp.clip(0.2 + 1.5999999 * jax.random.uniform(seeds[0], (GRID_Y, GRID_X, GRID_Z, LEVELS), jnp.float32) ** level_of(seeds[0], (GRID_Y, GRID_X, GRID_Z, LEVELS), ((0, 4), (1, 4), (2, 2)), -0.2, 0.2), 0.2, 1.8)
    flow_y = jnp.clip(jax.random.uniform(seeds[1], (GRID_Y, GRID_X, GRID_Z, LEVELS), jnp.float32, -0.3, 0.3) * level_of(seeds[1], (GRID_Y, GRID_X, GRID_Z, LEVELS), ((0, 4), (1, 4), (2, 2)), -0.4, 0.0), -0.3, 0.3)
    flow_x = jnp.clip(jax.random.uniform(seeds[2], (GRID_Y, GRID_X, GRID_Z, LEVELS), jnp.float32, -0.3, 0.3) * level_of(seeds[2], (GRID_Y, GRID_X, GRID_Z, LEVELS), ((0, 4), (1, 4), (2, 2)), -0.4, 0.0), -0.3, 0.3)
    flow_z = jnp.clip(jax.random.uniform(seeds[3], (GRID_Y, GRID_X, GRID_Z, LEVELS), jnp.float32, -0.3, 0.3) * level_of(seeds[3], (GRID_Y, GRID_X, GRID_Z, LEVELS), ((0, 4), (1, 4), (2, 2)), -0.4, 0.0), -0.3, 0.3)
    return {"field_values": field_values, "flow_y": flow_y, "flow_x": flow_x, "flow_z": flow_z}


def without_rim(values, dims):
    for dim in dims:
        values = lax.slice_in_dim(values, 1, values.shape[dim] - 1, axis=dim)
    return values


def shifted_cells(values, dim, start, dims):
    others = [other for other in dims if other != dim]
    values = without_rim(values, others)
    return lax.slice_in_dim(values, start, start + values.shape[dim] - 2, axis=dim)


def march_step(padded, flow_y, flow_x, flow_z):
    middle = without_rim(padded, (0, 1, 2))
    lower = [shifted_cells(padded, dim, 0, (0, 1, 2)) for dim in (0, 1, 2)]
    upper = [shifted_cells(padded, dim, 2, (0, 1, 2)) for dim in (0, 1, 2)]
    slopes = [above - below for above, below in zip(upper, lower)]
    smooth_rate = 0.05
    spread = lower[0] + upper[0] + lower[1] + upper[1] + lower[2] + upper[2] - 6.0 * middle
    return middle - flow_y * slopes[0] - flow_x * slopes[1] - flow_z * slopes[2] + smooth_rate * spread


def reference(field_values, flow_y, flow_x, flow_z):
    for step in range(STEPS):
        field_values = march_step(jnp.pad(field_values, ((1, 1), (1, 1), (1, 1), (0, 0)), mode="wrap"), flow_y, flow_x, flow_z)
    potential = jnp.cumsum(field_values, axis=2) / GRID_Z
    return potential, field_values
```

```python
import functools

import jax
import jax.numpy as jnp
from jax import lax
from jax.experimental import pallas as pl
from jax.experimental.pallas import tpu as pltpu
from jax.sharding import PartitionSpec as P

STEPS = 4
AXES = ("south", "east", "down")
MESH = pl.DeviceIdType.MESH


def group_of(columns):
    return next(size for size in (8, 4, 2, 1) if columns % size == 0)


def chunk_of(columns, group):
    return next(size for size in (2 * group, 2 * group, group) if columns % size == 0)


def kernel(sizes, depth, field, flow_y, flow_x, flow_z, pot, end, u, fy, fx, fz,
           faces, halos, totals, totals_in, load_sem, south_recv, east_recv, down_recv,
           tot_recv, south_send, east_send, down_send, tot_send, go):
    rows, cells, levels = field.shape
    columns = cells // depth
    group = group_of(columns)
    width = chunk_of(columns, group)
    chunks = columns // width
    places = {axis: lax.axis_index(axis) for axis in AXES}

    def beside(axis, hop):
        return {axis: lax.rem(places[axis] + hop, sizes[axis])}

    odd = lax.rem(places["south"], 2)
    near = odd
    leads = lax.rem(places["down"], 2) == 0
    follows = jnp.logical_not(leads)
    split = sizes["down"] == 2 and sizes["south"] % 2 == 0 and sizes["south"] > 2
    hops = [(axis, hop) for axis in ("south", "east") for hop in sorted({1, sizes[axis] - 1})]
    barrier = pltpu.get_barrier_semaphore()
    partner = beside("south", 1 + near * (sizes["south"] - 2))

    def greet(device_id):
        pl.semaphore_signal(barrier, inc=1, device_id=device_id, device_id_type=MESH)

    if split:
        @pl.when(leads)
        def _():
            greet(partner)
            greet({"down": 1})

        for axis, hop in hops:
            greet({**beside(axis, hop), "down": 1})
        greeted = jnp.where(leads, 1, 2 * len(hops) + 1)
    else:
        hops += [("down", hop) for hop in range(1, sizes["down"])]
        for axis, hop in hops:
            greet(beside(axis, hop))
        greeted = len(hops)

    def load(src, dst, sem):
        return pltpu.make_async_copy(src, dst, load_sem.at[sem])

    def done(ref, sem):
        pltpu.make_async_copy(ref, ref, sem).wait()

    def rows_of(t, start, count):
        return u.at[t, pl.ds(start, count), pl.ds(depth, cells), :]

    rims = [load(field.at[pl.ds(y, 1)], rows_of(0, y + 1, 1), 0) for y in (0, rows - 1)]
    inner = load(field.at[pl.ds(1, rows - 2)], rows_of(0, 2, rows - 2), 1)
    flows = [load(src, dst, 2) for src, dst in ((flow_y, fy), (flow_x, fx), (flow_z, fz))]
    for copy in rims:
        copy.start()
    done(rows_of(0, 1, 2), load_sem.at[0])
    inner.start()
    for copy in flows:
        copy.start()
    pl.semaphore_wait(barrier, greeted)

    def south(t, side, c):
        at = pl.multiple_of(c * width * depth, 8)
        return pltpu.make_async_remote_copy(
            src_ref=u.at[t, (1 - side) * (rows - 1) + 1, pl.ds(at + depth, width * depth), :],
            dst_ref=u.at[t, side * (rows + 1), pl.ds(at + depth, width * depth), :],
            send_sem=south_send, recv_sem=south_recv.at[t % 2, c],
            device_id=beside("south", 1 + side * (sizes["south"] - 2)), device_id_type=MESH)

    def south_done(t, c):
        at = pl.multiple_of(c * width * depth, 8)
        done(u.at[t, pl.ds(0, 2), pl.ds(at + depth, width * depth), :], south_recv.at[t % 2, c])

    blocks = ((1, rows - 2), (0, 1), (rows - 1, 1))

    def east(t, side, part):
        start, count = blocks[part]
        column = columns if side == 0 else 1
        if t == 0:
            src = field.at[pl.ds(start, count), pl.ds((column - 1) * depth, depth), :]
        else:
            src = u.at[t, pl.ds(start + 1, count), pl.ds(column * depth, depth), :]
        return pltpu.make_async_remote_copy(
            src_ref=src,
            dst_ref=u.at[t, pl.ds(start + 1, count), pl.ds(0 if side == 0 else cells + depth, depth), :],
            send_sem=east_send, recv_sem=east_recv.at[t % 2, min(part, 1)],
            device_id=beside("east", 1 if side == 0 else sizes["east"] - 1), device_id_type=MESH)

    def down(t, side, part):
        start, count = blocks[part]
        return pltpu.make_async_remote_copy(
            src_ref=faces.at[t, side, pl.ds(start, count)],
            dst_ref=halos.at[t, side, pl.ds(start, count)],
            send_sem=down_send, recv_sem=down_recv.at[t % 2, min(part, 1)],
            device_id=beside("down", 1 if side == 0 else sizes["down"] - 1), device_id_type=MESH)

    def sides_start(t, parts):
        for part in parts:
            for side in (0, 1):
                down(t, side, part).start()
                east(t, side, part).start()

    def sides_done(t, part):
        count = rows - 2 if part == 0 else 2
        done(u.at[t, pl.ds(0, count), pl.ds(0, 2 * depth), :], east_recv.at[t % 2, part])
        done(halos.at[t, :, pl.ds(0, count)], down_recv.at[t % 2, part])

    def total(hop, piece, y0, count, x0, span):
        cut = (pl.ds(y0, count), pl.ds(x0, span))
        return pltpu.make_async_remote_copy(
            src_ref=totals.at[cut], dst_ref=totals_in.at[(hop - 1, *cut)],
            send_sem=tot_send.at[hop - 1], recv_sem=tot_recv.at[hop - 1, piece],
            device_id=beside("down", hop), device_id_type=MESH)

    def rim_at(c):
        return pl.multiple_of(c * width, group)

    place_in_block = lax.broadcasted_iota(jnp.int32, (depth, levels), 0)
    on_first, on_last = place_in_block == 0, place_in_block == depth - 1

    def take_faces(t, y, x0):
        for side, place in ((0, depth - 1), (1, 0)):
            start = (x0 + 1) * depth + place
            faces[t, side, y, pl.ds(x0, group), :] = u[t, y + 1, pl.ds(start, group, stride=depth), :]

    def march(t, y, x0):
        def at(x, pad):
            return pl.ds(pl.multiple_of((x + pad) * depth, 8), depth)

        line = [u[t - 1, y + 1, at(x0 + g, 0), :] for g in range(group + 2)]
        for g in range(group):
            x = x0 + g
            mid, west, east_of = line[g + 1], line[g], line[g + 2]
            north, south_of = u[t - 1, y, at(x, 1), :], u[t - 1, y + 2, at(x, 1), :]
            low = jnp.broadcast_to(halos[t - 1, 0, y, pl.ds(x, 1), :], (depth, levels))
            high = jnp.broadcast_to(halos[t - 1, 1, y, pl.ds(x, 1), :], (depth, levels))
            low = jnp.where(on_first, low, pltpu.roll(mid, 1, 0))
            high = jnp.where(on_last, high, pltpu.roll(mid, depth - 1, 0))
            own = at(x, 0)
            spread = (north + south_of) + (west + east_of) + (low + high) - 6.0 * mid
            value = (mid - fy[y, own, :] * (south_of - north) - fx[y, own, :] * (east_of - west)
                     - fz[y, own, :] * (high - low) + 0.05 * spread)
            if t < STEPS:
                u[t, y + 1, at(x, 1), :] = value
            else:
                end[y, own, :] = value
                hop = 1
                while hop < depth:
                    value = value + jnp.where(place_in_block >= hop, pltpu.roll(value, hop, 0), 0.0)
                    hop *= 2
                pot[y, own, :] = value
        if t < STEPS:
            take_faces(t, y, x0)
        else:
            start = x0 * depth + depth - 1
            totals[y, pl.ds(x0, group), :] = pot[y, pl.ds(start, group, stride=depth), :]

    def over(y0, count, x0, span, body):
        groups = span // group

        def one(i, carry):
            body(y0 + i // groups, pl.multiple_of(x0 + (i % groups) * group, group))
            return carry

        lax.fori_loop(0, count * groups, one, 0)

    def finish(y, x0):
        for g in range(group):
            own = pl.ds(pl.multiple_of((x0 + g) * depth, 8), depth)
            value = pot[y, own, :]
            for hop in range(1, sizes["down"]):
                below = jnp.broadcast_to(totals_in[hop - 1, y, pl.ds(x0 + g, 1), :], (depth, levels))
                value = value + jnp.where(places["down"] >= hop, below, 0.0)
            pot[y, own, :] = value * (1.0 / (depth * sizes["down"]))

    down_hops = range(1, sizes["down"])

    def each(count, body):
        def one(i, carry):
            body(i)
            return carry

        lax.fori_loop(0, count, one, 0)

    def upwards(body):
        for hop in down_hops:
            pl.when(places["down"] + hop < sizes["down"])(functools.partial(body, hop))

    def from_below(body):
        for hop in down_hops:
            pl.when(places["down"] >= hop)(functools.partial(body, hop))

    def rim_over(c, body):
        groups = width // group

        def one(i):
            body((i // groups) * (rows - 1), pl.multiple_of(c * width + (i % groups) * group, group))

        each(2 * groups, one)

    def send_chunk(t, c):
        south(t, 1 - near, c).start()
        south(t, near, c).start()

    def send_first():
        each(chunks, lambda c: send_chunk(0, c))

    def send_rim_totals(c):
        def one(hop):
            for y in (0, rows - 1):
                total(hop, 1 + c, y, 1, rim_at(c), width).start()

        upwards(one)

    def finish_rim(c):
        from_below(lambda hop: done(totals_in.at[hop - 1, pl.ds(0, 2), pl.ds(rim_at(c), width)],
                                    tot_recv.at[hop - 1, 1 + c]))
        rim_over(c, finish)

    if split:
        @pl.when(leads)
        def _():
            each(chunks, lambda c: south(0, near, c).start())

        @pl.when(follows)
        def _():
            pl.semaphore_signal(go, inc=1, device_id={"down": 0}, device_id_type=MESH)
    else:
        pl.when(leads)(send_first)
    done(rows_of(0, 2, rows - 2), load_sem.at[1])
    over(0, rows, 0, columns, functools.partial(take_faces, 0))
    if split:
        @pl.when(leads)
        def _():
            pl.semaphore_wait(go, 1)
            each(chunks, lambda c: south(0, 1 - near, c).start())
    sides_start(0, (0, 1, 2))
    pl.when(follows)(send_first)
    done(u.at[pl.ds(0, 3), pl.ds(0, rows), pl.ds(depth, cells), :], load_sem.at[2])

    for t in range(1, STEPS + 1):
        sides_done(t - 1, 0)
        over(*blocks[0], 0, columns, functools.partial(march, t))
        if t < STEPS:
            sides_start(t, (0,))
        else:
            upwards(lambda hop: total(hop, 0, *blocks[0], 0, columns).start())
            from_below(lambda hop: total(hop, 0, *blocks[0], 0, columns).wait_recv())
            over(*blocks[0], 0, columns, finish)
        sides_done(t - 1, 1)

        def rim(c):
            south_done(t - 1, c)
            rim_over(c, functools.partial(march, t))
            if t < STEPS:
                send_chunk(t, c)
            else:
                send_rim_totals(c)
                pl.when(c > 0)(lambda: finish_rim(c - 1))

        each(chunks, rim)
        if t < STEPS:
            sides_start(t, (1, 2))
    finish_rim(chunks - 1)
    done(u.at[:, pl.ds(0, 2), pl.ds(depth, cells), :], south_send)
    done(u.at[:, pl.ds(0, rows), pl.ds(0, 2 * depth), :], east_send)
    done(faces, down_send)
    upwards(lambda hop: done(totals, tot_send.at[hop - 1]))


def write_out(*refs):
    count = len(refs) // 2
    sems = refs[-1]
    pairs = list(zip(refs[:count], refs[count:-1]))
    for i, (src, dst) in enumerate(pairs):
        for row in range(src.shape[0]):
            pltpu.make_async_copy(src.at[row], dst.at[row], sems.at[i]).start()
    for i, (src, dst) in enumerate(pairs):
        pltpu.make_async_copy(src, dst, sems.at[i]).wait()


def local(sizes, field_values, *flows):
    rows, columns, depth, levels = field_values.shape
    cells = columns * depth
    width = chunk_of(columns, group_of(columns))
    flat = [array.reshape(rows, cells, levels) for array in (field_values, *flows)]
    block = pltpu.VMEM((rows, cells, levels), jnp.float32)
    dma = pltpu.SemaphoreType.DMA
    others = sizes["down"] - 1
    face = (rows, columns, levels)
    out = jax.ShapeDtypeStruct((rows, cells, levels), jnp.float32)
    held = pl.pallas_call(
        functools.partial(kernel, sizes, depth),
        out_shape=(block, block),
        in_specs=[pl.BlockSpec(memory_space=pl.ANY)] * 4,
        out_specs=(pl.BlockSpec(memory_space=pltpu.VMEM),) * 2,
        scratch_shapes=[
            pltpu.VMEM((STEPS, rows + 2, cells + 2 * depth, levels), jnp.float32),
            block, block, block,
            pltpu.VMEM((STEPS, 2, *face), jnp.float32),
            pltpu.VMEM((STEPS, 2, *face), jnp.float32),
            pltpu.VMEM(face, jnp.float32),
            pltpu.VMEM((others, *face), jnp.float32),
            dma((3,)),
            dma((2, columns // width)), dma((2, 2)), dma((2, 2)), dma((others, 1 + columns // width)),
            dma, dma, dma, dma((others,)),
            pltpu.SemaphoreType.REGULAR,
        ],
        compiler_params=pltpu.CompilerParams(
            collective_id=0, has_side_effects=True, vmem_limit_bytes=48 * 1024 * 1024),
    )(*flat)
    results = pl.pallas_call(
        write_out,
        out_shape=(out, out),
        in_specs=[pl.BlockSpec(memory_space=pltpu.VMEM)] * 2,
        out_specs=(pl.BlockSpec(memory_space=pltpu.HBM),) * 2,
        scratch_shapes=[dma((2,))],
        compiler_params=pltpu.CompilerParams(vmem_limit_bytes=8 * 1024 * 1024),
    )(*held)
    return tuple(array.reshape(rows, columns, depth, levels) for array in results)


def solution(mesh):
    spec = P("south", "east", "down", None)
    sizes = {axis: mesh.shape[axis] for axis in AXES}
    return jax.shard_map(
        functools.partial(local, sizes), mesh=mesh, in_specs=(spec,) * 4,
        out_specs=(spec, spec), check_vma=False)
```

```python
import functools

import jax
import jax.numpy as jnp
from jax import lax
from jax.experimental import pallas as pl
from jax.experimental.pallas import tpu as pltpu
from jax.sharding import PartitionSpec as P

STEPS = 4
AXES = ("south", "east", "down")
MESH = pl.DeviceIdType.MESH


def group_of(columns):
    return next(size for size in (8, 4, 2, 1) if columns % size == 0)


def chunk_of(columns, group):
    return next(size for size in (2 * group, 2 * group, group) if columns % size == 0)


def kernel(sizes, depth, field, flow_y, flow_x, flow_z, pot, end, u, fy, fx, fz,
           faces, halos, totals, totals_in, load_sem, south_recv, east_recv, down_recv,
           tot_recv, south_send, east_send, down_send, tot_send, go):
    rows, cells, levels = field.shape
    columns = cells // depth
    group = group_of(columns)
    width = chunk_of(columns, group)
    chunks = columns // width
    places = {axis: lax.axis_index(axis) for axis in AXES}

    def beside(axis, hop):
        return {axis: lax.rem(places[axis] + hop, sizes[axis])}

    odd = lax.rem(places["south"], 2)
    near = odd
    leads = lax.rem(places["down"], 2) == 0
    follows = jnp.logical_not(leads)
    split = sizes["down"] == 2 and sizes["south"] % 2 == 0 and sizes["south"] > 2
    hops = [(axis, hop) for axis in ("south", "east") for hop in sorted({1, sizes[axis] - 1})]
    barrier = pltpu.get_barrier_semaphore()
    partner = beside("south", 1 + near * (sizes["south"] - 2))

    def greet(device_id):
        pl.semaphore_signal(barrier, inc=1, device_id=device_id, device_id_type=MESH)

    if split:
        @pl.when(follows)
        def _():
            greet(partner)
            greet({"down": 0})

        for axis, hop in hops:
            greet({**beside(axis, hop), "down": 0})
        greeted = jnp.where(follows, 1, 2 * len(hops) + 1)
    else:
        hops += [("down", hop) for hop in range(1, sizes["down"])]
        for axis, hop in hops:
            greet(beside(axis, hop))
        greeted = len(hops)

    def load(src, dst, sem):
        return pltpu.make_async_copy(src, dst, load_sem.at[sem])

    def done(ref, sem):
        pltpu.make_async_copy(ref, ref, sem).wait()

    def rows_of(t, start, count):
        return u.at[t, pl.ds(start, count), pl.ds(depth, cells), :]

    def rim_piece(side, start, count, sem):
        y = (1 - side) * (rows - 1)
        return load(field.at[y, pl.ds(start, count)], u.at[0, y + 1, pl.ds(depth + start, count), :], sem)

    early = min(1, chunks)
    head = early * width * depth
    rest = [rim_piece(1 - near, 0, cells, 1)]
    if head < cells:
        rest.append(rim_piece(near, head, cells - head, 1))
    inner = load(field.at[pl.ds(1, rows - 2)], rows_of(0, 2, rows - 2), 2)
    flows = [load(src, dst, 3) for src, dst in ((flow_y, fy), (flow_x, fx), (flow_z, fz))]
    rim_piece(near, 0, head, 0).start()
    for copy in rest:
        copy.start()
    done(u.at[0, 0, pl.ds(0, head), :], load_sem.at[0])
    inner.start()
    for copy in flows:
        copy.start()
    pl.semaphore_wait(barrier, greeted)

    def south(t, side, c):
        at = pl.multiple_of(c * width * depth, 8)
        return pltpu.make_async_remote_copy(
            src_ref=u.at[t, (1 - side) * (rows - 1) + 1, pl.ds(at + depth, width * depth), :],
            dst_ref=u.at[t, side * (rows + 1), pl.ds(at + depth, width * depth), :],
            send_sem=south_send, recv_sem=south_recv.at[t % 2, c],
            device_id=beside("south", 1 + side * (sizes["south"] - 2)), device_id_type=MESH)

    def south_done(t, c):
        at = pl.multiple_of(c * width * depth, 8)
        done(u.at[t, pl.ds(0, 2), pl.ds(at + depth, width * depth), :], south_recv.at[t % 2, c])

    def rest_done():
        done(u.at[pl.ds(0, 2), 0, pl.ds(0, cells - head // 2), :], load_sem.at[1])

    blocks = ((1, rows - 2), (0, 1), (rows - 1, 1))

    def east(t, side, part):
        start, count = blocks[part]
        column = columns if side == 0 else 1
        if t == 0:
            src = field.at[pl.ds(start, count), pl.ds((column - 1) * depth, depth), :]
        else:
            src = u.at[t, pl.ds(start + 1, count), pl.ds(column * depth, depth), :]
        return pltpu.make_async_remote_copy(
            src_ref=src,
            dst_ref=u.at[t, pl.ds(start + 1, count), pl.ds(0 if side == 0 else cells + depth, depth), :],
            send_sem=east_send, recv_sem=east_recv.at[t % 2, min(part, 1)],
            device_id=beside("east", 1 if side == 0 else sizes["east"] - 1), device_id_type=MESH)

    def down(t, side, part):
        start, count = blocks[part]
        return pltpu.make_async_remote_copy(
            src_ref=faces.at[t, side, pl.ds(start, count)],
            dst_ref=halos.at[t, side, pl.ds(start, count)],
            send_sem=down_send, recv_sem=down_recv.at[t % 2, min(part, 1)],
            device_id=beside("down", 1 if side == 0 else sizes["down"] - 1), device_id_type=MESH)

    def sides_start(t, parts):
        for part in parts:
            for side in (0, 1):
                down(t, side, part).start()
                east(t, side, part).start()

    def sides_done(t, part):
        count = rows - 2 if part == 0 else 2
        done(u.at[t, pl.ds(0, count), pl.ds(0, 2 * depth), :], east_recv.at[t % 2, part])
        done(halos.at[t, :, pl.ds(0, count)], down_recv.at[t % 2, part])

    def total(hop, piece, y0, count, x0, span):
        cut = (pl.ds(y0, count), pl.ds(x0, span))
        return pltpu.make_async_remote_copy(
            src_ref=totals.at[cut], dst_ref=totals_in.at[(hop - 1, *cut)],
            send_sem=tot_send.at[hop - 1], recv_sem=tot_recv.at[hop - 1, piece],
            device_id=beside("down", hop), device_id_type=MESH)

    def rim_at(c):
        return pl.multiple_of(c * width, group)

    place_in_block = lax.broadcasted_iota(jnp.int32, (depth, levels), 0)
    on_first, on_last = place_in_block == 0, place_in_block == depth - 1

    def take_faces(t, y, x0):
        for side, place in ((0, depth - 1), (1, 0)):
            start = (x0 + 1) * depth + place
            faces[t, side, y, pl.ds(x0, group), :] = u[t, y + 1, pl.ds(start, group, stride=depth), :]

    def march(t, y, x0):
        def at(x, pad):
            return pl.ds(pl.multiple_of((x + pad) * depth, 8), depth)

        line = [u[t - 1, y + 1, at(x0 + g, 0), :] for g in range(group + 2)]
        for g in range(group):
            x = x0 + g
            mid, west, east_of = line[g + 1], line[g], line[g + 2]
            north, south_of = u[t - 1, y, at(x, 1), :], u[t - 1, y + 2, at(x, 1), :]
            low = jnp.broadcast_to(halos[t - 1, 0, y, pl.ds(x, 1), :], (depth, levels))
            high = jnp.broadcast_to(halos[t - 1, 1, y, pl.ds(x, 1), :], (depth, levels))
            low = jnp.where(on_first, low, pltpu.roll(mid, 1, 0))
            high = jnp.where(on_last, high, pltpu.roll(mid, depth - 1, 0))
            own = at(x, 0)
            spread = (north + south_of) + (west + east_of) + (low + high) - 6.0 * mid
            value = (mid - fy[y, own, :] * (south_of - north) - fx[y, own, :] * (east_of - west)
                     - fz[y, own, :] * (high - low) + 0.05 * spread)
            if t < STEPS:
                u[t, y + 1, at(x, 1), :] = value
            else:
                end[y, own, :] = value
                hop = 1
                while hop < depth:
                    value = value + jnp.where(place_in_block >= hop, pltpu.roll(value, hop, 0), 0.0)
                    hop *= 2
                pot[y, own, :] = value
        if t < STEPS:
            take_faces(t, y, x0)
        else:
            start = x0 * depth + depth - 1
            totals[y, pl.ds(x0, group), :] = pot[y, pl.ds(start, group, stride=depth), :]

    def over(y0, count, x0, span, body):
        groups = span // group

        def one(i, carry):
            body(y0 + i // groups, pl.multiple_of(x0 + (i % groups) * group, group))
            return carry

        lax.fori_loop(0, count * groups, one, 0)

    def finish(y, x0):
        for g in range(group):
            own = pl.ds(pl.multiple_of((x0 + g) * depth, 8), depth)
            value = pot[y, own, :]
            for hop in range(1, sizes["down"]):
                below = jnp.broadcast_to(totals_in[hop - 1, y, pl.ds(x0 + g, 1), :], (depth, levels))
                value = value + jnp.where(places["down"] >= hop, below, 0.0)
            pot[y, own, :] = value * (1.0 / (depth * sizes["down"]))

    down_hops = range(1, sizes["down"])

    def each(count, body):
        def one(i, carry):
            body(i)
            return carry

        lax.fori_loop(0, count, one, 0)

    def upwards(body):
        for hop in down_hops:
            pl.when(places["down"] + hop < sizes["down"])(functools.partial(body, hop))

    def from_below(body):
        for hop in down_hops:
            pl.when(places["down"] >= hop)(functools.partial(body, hop))

    def rim_over(c, body):
        groups = width // group

        def one(i):
            body((i // groups) * (rows - 1), pl.multiple_of(c * width + (i % groups) * group, group))

        each(2 * groups, one)

    def send_chunk(t, c):
        south(t, 1 - near, c).start()
        south(t, near, c).start()

    last_block = sizes["south"] - 1
    first = jnp.where(places["south"] == last_block, 0, jnp.where(places["south"] == 1, 1, 1 - near))
    lag = min(4, chunks)

    def send_last(c):
        south(STEPS - 1, first, c).start()
        pl.when(c >= lag)(lambda: south(STEPS - 1, 1 - first, c - lag).start())

    def send_first():
        each(chunks, lambda c: send_chunk(0, c))

    def send_rim_totals(c):
        def one(hop):
            for y in (0, rows - 1):
                total(hop, 1 + c, y, 1, rim_at(c), width).start()

        upwards(one)

    def finish_rim(c):
        from_below(lambda hop: done(totals_in.at[hop - 1, pl.ds(0, 2), pl.ds(rim_at(c), width)],
                                    tot_recv.at[hop - 1, 1 + c]))
        rim_over(c, finish)

    def send_far():
        each(chunks, lambda c: south(0, 1 - near, c).start())

    if split:
        @pl.when(follows)
        def _():
            each(early, lambda c: south(0, near, c).start())

        @pl.when(leads)
        def _():
            pl.semaphore_signal(go, inc=1, device_id={"down": 1}, device_id_type=MESH)

        rest_done()

        @pl.when(follows)
        def _():
            each(chunks - early, lambda c: south(0, near, early + c).start())
    else:
        rest_done()
    pl.when(leads)(send_first)
    done(rows_of(0, 2, rows - 2), load_sem.at[2])
    over(0, rows, 0, columns, functools.partial(take_faces, 0))
    if split:
        pl.when(follows)(lambda: pl.semaphore_wait(go, 1))
    sides_start(0, (0, 1, 2))
    if not split:
        pl.when(follows)(send_first)
    done(u.at[pl.ds(0, 3), pl.ds(0, rows), pl.ds(depth, cells), :], load_sem.at[3])

    ahead = min(3, chunks) if split else 0
    if split:
        @pl.when(leads)
        def _():
            each(ahead, lambda c: south_done(0, c))
            pl.semaphore_signal(go, inc=1, device_id={"down": 1}, device_id_type=MESH)

    def take_south(t, c):
        if t == 0 and split:
            pl.when(jnp.logical_or(follows, c >= ahead))(lambda: south_done(t, c))
        else:
            south_done(t, c)

    for t in range(1, STEPS + 1):
        sides_done(t - 1, 0)
        over(*blocks[0], 0, columns, functools.partial(march, t))
        if t == 1 and split:
            @pl.when(follows)
            def _():
                pl.semaphore_wait(go, 1)
                send_far()

        if t < STEPS:
            sides_start(t, (0,))
        else:
            upwards(lambda hop: total(hop, 0, *blocks[0], 0, columns).start())
            from_below(lambda hop: total(hop, 0, *blocks[0], 0, columns).wait_recv())
            over(*blocks[0], 0, columns, finish)
        sides_done(t - 1, 1)

        def rim(c):
            take_south(t - 1, c)
            rim_over(c, functools.partial(march, t))
            if t < STEPS - 1:
                send_chunk(t, c)
            elif t < STEPS:
                send_last(c)
            else:
                send_rim_totals(c)
                pl.when(c > 0)(lambda: finish_rim(c - 1))

        each(chunks, rim)
        if t == STEPS - 1:
            each(lag, lambda c: south(t, 1 - first, chunks - lag + c).start())
        if t < STEPS:
            sides_start(t, (1, 2))
    finish_rim(chunks - 1)
    done(u.at[:, pl.ds(0, 2), pl.ds(depth, cells), :], south_send)
    done(u.at[:, pl.ds(0, rows), pl.ds(0, 2 * depth), :], east_send)
    done(faces, down_send)
    upwards(lambda hop: done(totals, tot_send.at[hop - 1]))


def write_out(*refs):
    count = len(refs) // 2
    sems = refs[-1]
    pairs = list(zip(refs[:count], refs[count:-1]))
    for i, (src, dst) in enumerate(pairs):
        for row in range(src.shape[0]):
            pltpu.make_async_copy(src.at[row], dst.at[row], sems.at[i]).start()
    for i, (src, dst) in enumerate(pairs):
        pltpu.make_async_copy(src, dst, sems.at[i]).wait()


def local(sizes, field_values, *flows):
    rows, columns, depth, levels = field_values.shape
    cells = columns * depth
    width = chunk_of(columns, group_of(columns))
    flat = [array.reshape(rows, cells, levels) for array in (field_values, *flows)]
    block = pltpu.VMEM((rows, cells, levels), jnp.float32)
    dma = pltpu.SemaphoreType.DMA
    others = sizes["down"] - 1
    face = (rows, columns, levels)
    out = jax.ShapeDtypeStruct((rows, cells, levels), jnp.float32)
    held = pl.pallas_call(
        functools.partial(kernel, sizes, depth),
        out_shape=(block, block),
        in_specs=[pl.BlockSpec(memory_space=pl.ANY)] * 4,
        out_specs=(pl.BlockSpec(memory_space=pltpu.VMEM),) * 2,
        scratch_shapes=[
            pltpu.VMEM((STEPS, rows + 2, cells + 2 * depth, levels), jnp.float32),
            block, block, block,
            pltpu.VMEM((STEPS, 2, *face), jnp.float32),
            pltpu.VMEM((STEPS, 2, *face), jnp.float32),
            pltpu.VMEM(face, jnp.float32),
            pltpu.VMEM((others, *face), jnp.float32),
            dma((4,)),
            dma((2, columns // width)), dma((2, 2)), dma((2, 2)), dma((others, 1 + columns // width)),
            dma, dma, dma, dma((others,)),
            pltpu.SemaphoreType.REGULAR,
        ],
        compiler_params=pltpu.CompilerParams(
            collective_id=0, has_side_effects=True, vmem_limit_bytes=48 * 1024 * 1024),
    )(*flat)
    results = pl.pallas_call(
        write_out,
        out_shape=(out, out),
        in_specs=[pl.BlockSpec(memory_space=pltpu.VMEM)] * 2,
        out_specs=(pl.BlockSpec(memory_space=pltpu.HBM),) * 2,
        scratch_shapes=[dma((2,))],
        compiler_params=pltpu.CompilerParams(vmem_limit_bytes=8 * 1024 * 1024),
    )(*held)
    return tuple(array.reshape(rows, columns, depth, levels) for array in results)


def solution(mesh):
    spec = P("south", "east", "down", None)
    sizes = {axis: mesh.shape[axis] for axis in AXES}
    return jax.shard_map(
        functools.partial(local, sizes), mesh=mesh, in_specs=(spec,) * 4,
        out_specs=(spec, spec), check_vma=False)
```

```python
import functools

import jax
import jax.numpy as jnp
from jax import lax
from jax.experimental import pallas as pl
from jax.experimental.pallas import tpu as pltpu
from jax.sharding import PartitionSpec as P

STEPS = 4
AXES = ("south", "east", "down")
MESH = pl.DeviceIdType.MESH


def group_of(columns):
    return next(size for size in (8, 4, 2, 1) if columns % size == 0)


def chunk_of(columns, group):
    return next(size for size in (2 * group, group) if columns % size == 0)


def each(count, body):
    def one(i, carry):
        body(i)
        return carry

    lax.fori_loop(0, count, one, 0)


def new_values(depth, group, u, halos, fy, fx, fz, t, y, row, x0):
    levels = u.shape[-1]
    place = lax.broadcasted_iota(jnp.int32, (depth, levels), 0)

    def at(x, pad):
        return pl.ds(pl.multiple_of((x + pad) * depth, 8), depth)

    line = [u[t - 1, y + 1, at(x0 + g, 0), :] for g in range(group + 2)]
    values = []
    for g in range(group):
        x = x0 + g
        mid, west, east_of = line[g + 1], line[g], line[g + 2]
        north, south_of = u[t - 1, y, at(x, 1), :], u[t - 1, y + 2, at(x, 1), :]
        low = jnp.broadcast_to(halos[t - 1, 0, row, pl.ds(x, 1), :], (depth, levels))
        high = jnp.broadcast_to(halos[t - 1, 1, row, pl.ds(x, 1), :], (depth, levels))
        low = jnp.where(place == 0, low, pltpu.roll(mid, 1, 0))
        high = jnp.where(place == depth - 1, high, pltpu.roll(mid, depth - 1, 0))
        own = at(x, 0)
        spread = (north + south_of) + (west + east_of) + (low + high) - 6.0 * mid
        values.append(mid - fy[row, own, :] * (south_of - north) - fx[row, own, :] * (east_of - west)
                      - fz[row, own, :] * (high - low) + 0.05 * spread)
    return values


def running_sum(value):
    depth = value.shape[0]
    place = lax.broadcasted_iota(jnp.int32, value.shape, 0)
    hop = 1
    while hop < depth:
        value = value + jnp.where(place >= hop, pltpu.roll(value, hop, 0), 0.0)
        hop *= 2
    return value


def finished(sizes, totals_in, row, x, value):
    rank = lax.axis_index("down")
    for hop in range(1, sizes["down"]):
        below = jnp.broadcast_to(totals_in[hop - 1, row, pl.ds(x, 1), :], value.shape)
        value = value + jnp.where(rank >= hop, below, 0.0)
    return value * (1.0 / (value.shape[0] * sizes["down"]))


def kernel(sizes, depth, field, flow_y, flow_x, flow_z, pot, end, last_u, last_flows, last_halos, last_totals,
           u, fy, fx, fz, faces, halos, totals, totals_in, load_sem, south_recv, side_recv, tot_recv, south_send, side_send, tot_send, go):
    rows, cells, levels = field.shape
    columns = cells // depth
    group = group_of(columns)
    width = chunk_of(columns, group)
    chunks = columns // width
    places = {axis: lax.axis_index(axis) for axis in AXES}

    def beside(axis, hop):
        return {axis: lax.rem(places[axis] + hop, sizes[axis])}

    near = lax.rem(places["south"], 2)
    leads = lax.rem(places["down"], 2) == 0
    follows = jnp.logical_not(leads)
    split = sizes["down"] == 2 and sizes["south"] % 2 == 0 and sizes["south"] > 2
    hops = [(axis, hop) for axis in ("south", "east") for hop in sorted({1, sizes[axis] - 1})]
    barrier = pltpu.get_barrier_semaphore()
    partner = beside("south", 1 + near * (sizes["south"] - 2))

    def greet(device_id):
        pl.semaphore_signal(barrier, inc=1, device_id=device_id, device_id_type=MESH)

    if split:
        @pl.when(follows)
        def _():
            greet(partner)
            greet({"down": 0})

        for axis, hop in hops:
            greet({**beside(axis, hop), "down": 0})
        greeted = jnp.where(follows, 1, 2 * len(hops) + 1)
    else:
        hops += [("down", hop) for hop in range(1, sizes["down"])]
        for axis, hop in hops:
            greet(beside(axis, hop))
        greeted = len(hops)

    def load(src, dst, sem):
        return pltpu.make_async_copy(src, dst, load_sem.at[sem])

    def done(ref, sem):
        pltpu.make_async_copy(ref, ref, sem).wait()

    def rim_piece(side, start, count, sem):
        y = (1 - side) * (rows - 1)
        return load(field.at[y, pl.ds(start, count)], u.at[0, y + 1, pl.ds(depth + start, count), :], sem)

    early = min(1, chunks)
    head = early * width * depth
    rest = [rim_piece(1 - near, 0, cells, 1)]
    if head < cells:
        rest.append(rim_piece(near, head, cells - head, 1))
    inner = load(field.at[pl.ds(1, rows - 2)], u.at[0, pl.ds(2, rows - 2), pl.ds(depth, cells), :], 2)
    flows = [load(src, dst, 3) for src, dst in ((flow_y, fy), (flow_x, fx), (flow_z, fz))]
    rim_piece(near, 0, head, 0).start()
    for copy in rest:
        copy.start()
    done(u.at[0, 0, pl.ds(0, head), :], load_sem.at[0])
    inner.start()
    for copy in flows:
        copy.start()
    pl.semaphore_wait(barrier, greeted)

    def rest_done():
        done(u.at[pl.ds(0, 2), 0, pl.ds(0, cells - head // 2), :], load_sem.at[1])

    def chunk_at(c):
        return pl.ds(pl.multiple_of(c * width * depth + depth, 8), width * depth)

    def south(t, side, c):
        return pltpu.make_async_remote_copy(
            src_ref=u.at[t, (1 - side) * (rows - 1) + 1, chunk_at(c), :],
            dst_ref=u.at[t, side * (rows + 1), chunk_at(c), :],
            send_sem=south_send, recv_sem=south_recv.at[t % 2, c],
            device_id=beside("south", 1 + side * (sizes["south"] - 2)), device_id_type=MESH)

    def south_done(t, c):
        done(u.at[t, pl.ds(0, 2), chunk_at(c), :], south_recv.at[t % 2, c])

    blocks = ((1, rows - 2), (0, 1), (rows - 1, 1))

    def east(t, side, part):
        start, count = blocks[part]
        column = columns if side == 0 else 1
        if t == 0:
            src = field.at[pl.ds(start, count), pl.ds((column - 1) * depth, depth), :]
        else:
            src = u.at[t, pl.ds(start + 1, count), pl.ds(column * depth, depth), :]
        return pltpu.make_async_remote_copy(
            src_ref=src,
            dst_ref=u.at[t, pl.ds(start + 1, count), pl.ds(0 if side == 0 else cells + depth, depth), :],
            send_sem=side_send, recv_sem=side_recv.at[t % 2, min(part, 1)],
            device_id=beside("east", 1 if side == 0 else sizes["east"] - 1), device_id_type=MESH)

    def down(t, side, part):
        start, count = blocks[part]
        return pltpu.make_async_remote_copy(
            src_ref=faces.at[t, side, pl.ds(start, count)],
            dst_ref=halos.at[t, side, pl.ds(start, count)],
            send_sem=side_send, recv_sem=side_recv.at[t % 2, min(part, 1)],
            device_id=beside("down", 1 if side == 0 else sizes["down"] - 1), device_id_type=MESH)

    def sides_start(t, parts):
        for part in parts:
            for side in (0, 1):
                down(t, side, part).start()
                east(t, side, part).start()

    both = 2 * (depth + columns)

    def sides_done(t, part):
        done(u.at[t, pl.ds(0, rows - 2 if part == 0 else 2), pl.ds(0, both), :], side_recv.at[t % 2, part])

    def total(hop, piece, y0, count, x0, span):
        cut = (pl.ds(y0, count), pl.ds(x0, span))
        return pltpu.make_async_remote_copy(
            src_ref=totals.at[cut], dst_ref=totals_in.at[(hop - 1, *cut)],
            send_sem=tot_send.at[hop - 1], recv_sem=tot_recv.at[hop - 1, piece],
            device_id=beside("down", hop), device_id_type=MESH)

    def rim_at(c):
        return pl.multiple_of(c * width, group)

    def take_faces(t, y, x0):
        for side, place in ((0, depth - 1), (1, 0)):
            start = (x0 + 1) * depth + place
            faces[t, side, y, pl.ds(x0, group), :] = u[t, y + 1, pl.ds(start, group, stride=depth), :]

    def march(t, y, x0):
        values = new_values(depth, group, u, halos, fy, fx, fz, t, y, y, x0)
        for g, value in enumerate(values):
            if t < STEPS:
                u[t, y + 1, pl.ds(pl.multiple_of((x0 + g + 1) * depth, 8), depth), :] = value
            else:
                own = pl.ds(pl.multiple_of((x0 + g) * depth, 8), depth)
                end[y, own, :] = value
                pot[y, own, :] = running_sum(value)
        if t < STEPS:
            take_faces(t, y, x0)
        else:
            start = x0 * depth + depth - 1
            totals[y, pl.ds(x0, group), :] = pot[y, pl.ds(start, group, stride=depth), :]

    def over(y0, count, x0, span, body):
        groups = span // group
        each(count * groups,
             lambda i: body(y0 + i // groups, pl.multiple_of(x0 + (i % groups) * group, group)))

    def finish(y, x0):
        for g in range(group):
            own = pl.ds(pl.multiple_of((x0 + g) * depth, 8), depth)
            pot[y, own, :] = finished(sizes, totals_in, y, x0 + g, pot[y, own, :])

    down_hops = range(1, sizes["down"])
    last_rank = sizes["down"] - 1

    def upwards(body):
        for hop in down_hops:
            pl.when(places["down"] + hop <= last_rank)(functools.partial(body, hop))

    def from_below(body):
        for hop in down_hops:
            pl.when(places["down"] >= hop)(functools.partial(body, hop))

    def rim_over(c, body):
        groups = width // group
        each(2 * groups, lambda i: body((i // groups) * (rows - 1),
                                        pl.multiple_of(c * width + (i % groups) * group, group)))

    last_block = sizes["south"] - 1
    first = jnp.where(places["south"] == last_block, 0, jnp.where(places["south"] == 1, 1, 1 - near))
    lag = min(4, chunks)

    def send_chunk(t, c):
        south(t, 1 - near, c).start()
        south(t, near, c).start()

    def send_last(c):
        south(STEPS - 1, first, c).start()
        pl.when(c >= lag)(lambda: south(STEPS - 1, 1 - first, c - lag).start())

    def send_first():
        each(chunks, lambda c: send_chunk(0, c))

    def send_far():
        each(chunks, lambda c: south(0, 1 - near, c).start())

    def send_rim_totals(c):
        def one(hop):
            for y in (0, rows - 1):
                total(hop, 1 + c, y, 1, rim_at(c), width).start()

        upwards(one)

    def take_rim_totals(c):
        from_below(lambda hop: done(totals_in.at[hop - 1, pl.ds(0, 2), pl.ds(rim_at(c), width)],
                                    tot_recv.at[hop - 1, 1 + c]))

    def finish_rim(c):
        take_rim_totals(c)
        rim_over(c, finish)

    base = columns - width
    last_cells = pl.ds(base * depth, width * depth)

    def keep_last():
        for side in (0, 1):
            row = side * (rows - 1)
            for i in (0, 1, 2):
                if (side, i) not in ((0, 0), (1, 2)):
                    last_u[0, 3 * side + i] = u[STEPS - 1, row + i, pl.ds(base * depth, (width + 2) * depth), :]
            for i, flow in enumerate((fy, fx, fz)):
                last_flows[i, side] = flow[row, last_cells, :]
            for z in (0, 1):
                last_halos[0, z, side] = halos[STEPS - 1, z, row, pl.ds(base, width), :]

    def keep_south():
        for side in (0, 1):
            last_u[0, 5 * side, pl.ds(depth, width * depth), :] = u[
                STEPS - 1, side * (rows + 1), pl.ds((base + 1) * depth, width * depth), :]

    def keep_totals():
        for hop in down_hops:
            for side in (0, 1):
                @pl.when(places["down"] >= hop)
                def _():
                    last_totals[hop - 1, side] = totals_in[hop - 1, side * (rows - 1), pl.ds(base, width), :]

                @pl.when(places["down"] < hop)
                def _():
                    last_totals[hop - 1, side] = jnp.zeros((width, levels), jnp.float32)

    if split:
        @pl.when(follows)
        def _():
            each(early, lambda c: south(0, near, c).start())

        @pl.when(leads)
        def _():
            pl.semaphore_signal(go, inc=1, device_id={"down": 1}, device_id_type=MESH)

        rest_done()

        @pl.when(follows)
        def _():
            each(chunks - early, lambda c: south(0, near, early + c).start())
    else:
        rest_done()
    pl.when(leads)(send_first)
    done(u.at[0, pl.ds(2, rows - 2), pl.ds(depth, cells), :], load_sem.at[2])
    over(0, rows, 0, columns, functools.partial(take_faces, 0))
    if split:
        pl.when(follows)(lambda: pl.semaphore_wait(go, 1))
    sides_start(0, (0, 1, 2))
    if not split:
        pl.when(follows)(send_first)
    done(u.at[pl.ds(0, 3), pl.ds(0, rows), pl.ds(depth, cells), :], load_sem.at[3])

    ahead = min(3, chunks) if split else 0
    if split:
        @pl.when(leads)
        def _():
            each(ahead, lambda c: south_done(0, c))
            pl.semaphore_signal(go, inc=1, device_id={"down": 1}, device_id_type=MESH)

    def take_south(t, c):
        if t == 0 and split:
            pl.when(jnp.logical_or(follows, c >= ahead))(lambda: south_done(t, c))
        else:
            south_done(t, c)

    for t in range(1, STEPS + 1):
        sides_done(t - 1, 0)
        over(*blocks[0], 0, columns, functools.partial(march, t))
        if t == 1 and split:
            @pl.when(follows)
            def _():
                pl.semaphore_wait(go, 1)
                send_far()

        if t < STEPS:
            sides_start(t, (0,))
        else:
            upwards(lambda hop: total(hop, 0, *blocks[0], 0, columns).start())
            from_below(lambda hop: total(hop, 0, *blocks[0], 0, columns).wait_recv())
            over(*blocks[0], 0, columns, finish)
        sides_done(t - 1, 1)

        def rim(c):
            if t < STEPS:
                take_south(t - 1, c)
                rim_over(c, functools.partial(march, t))
                if t < STEPS - 1:
                    send_chunk(t, c)
                else:
                    send_last(c)
            else:
                pl.when(c > 0)(lambda: finish_rim(c - 1))
                pl.when(c == chunks - 1)(keep_last)
                take_south(t - 1, c)

                @pl.when(jnp.logical_or(c < chunks - 1, places["down"] < last_rank))
                def _():
                    rim_over(c, functools.partial(march, t))
                    send_rim_totals(c)

        each(chunks, rim)
        if t == STEPS - 1:
            each(lag, lambda c: south(t, 1 - first, chunks - lag + c).start())
        if t < STEPS:
            sides_start(t, (1, 2))
    keep_south()
    take_rim_totals(chunks - 1)
    keep_totals()
    done(u.at[:, pl.ds(0, 2), pl.ds(depth, cells), :], south_send)
    done(u.at[:, pl.ds(0, rows), pl.ds(0, both), :], side_send)
    upwards(lambda hop: done(totals, tot_send.at[hop - 1]))


def write_out(sizes, depth, pot, end, last_u, last_flows, last_halos, last_totals, pot_out, end_out,
              last_pot, last_end, sems):
    rows, cells, levels = pot.shape
    columns = cells // depth
    group = group_of(columns)
    width = chunk_of(columns, group)
    kept = cells - width * depth
    whole = ((pot, pot_out), (end, end_out))
    for i, (src, dst) in enumerate(whole):
        for y in range(1, rows - 1):
            pltpu.make_async_copy(src.at[y], dst.at[y], sems.at[i]).start()
        if kept:
            for y in (0, rows - 1):
                cut = (y, pl.ds(0, kept))
                pltpu.make_async_copy(src.at[cut], dst.at[cut], sems.at[i]).start()
    groups = width // group

    def last(i):
        side, x0 = i // groups, pl.multiple_of((i % groups) * group, group)
        values = new_values(depth, group, last_u, last_halos, *(last_flows.at[k] for k in (0, 1, 2)), 1, 3 * side, side, x0)
        for g, value in enumerate(values):
            own = pl.ds(pl.multiple_of((x0 + g) * depth, 8), depth)
            last_end[side, own, :] = value
            last_pot[side, own, :] = finished(sizes, last_totals, side, x0 + g, running_sum(value))

    each(2 * groups, last)
    for i, (src, (_, dst)) in enumerate(zip((last_pot, last_end), whole)):
        for side, y in ((0, 0), (1, rows - 1)):
            cut = (y, pl.ds(kept, cells - kept))
            pltpu.make_async_copy(src.at[side], dst.at[cut], sems.at[i]).start()
    for i, (src, dst) in enumerate(whole):
        pltpu.make_async_copy(src, dst, sems.at[i]).wait()


def local(sizes, field_values, *flows):
    rows, columns, depth, levels = field_values.shape
    cells = columns * depth
    width = chunk_of(columns, group_of(columns))
    flat = [array.reshape(rows, cells, levels) for array in (field_values, *flows)]
    block = pltpu.VMEM((rows, cells, levels), jnp.float32)
    dma = pltpu.SemaphoreType.DMA
    others = sizes["down"] - 1
    face = (rows, columns, levels)
    out = jax.ShapeDtypeStruct((rows, cells, levels), jnp.float32)
    in_vmem = pl.BlockSpec(memory_space=pltpu.VMEM)
    last = pltpu.VMEM((2, width * depth, levels), jnp.float32)
    held_shapes = (
        block, block,
        pltpu.VMEM((1, 6, (width + 2) * depth, levels), jnp.float32),
        pltpu.VMEM((3, 2, width * depth, levels), jnp.float32),
        pltpu.VMEM((1, 2, 2, width, levels), jnp.float32),
        pltpu.VMEM((others, 2, width, levels), jnp.float32),
    )
    held = pl.pallas_call(
        functools.partial(kernel, sizes, depth),
        out_shape=held_shapes,
        in_specs=[pl.BlockSpec(memory_space=pl.ANY)] * 4,
        out_specs=(in_vmem,) * len(held_shapes),
        scratch_shapes=[
            pltpu.VMEM((STEPS, rows + 2, cells + 2 * depth, levels), jnp.float32),
            block, block, block,
            pltpu.VMEM((STEPS, 2, *face), jnp.float32),
            pltpu.VMEM((STEPS, 2, *face), jnp.float32),
            pltpu.VMEM(face, jnp.float32),
            pltpu.VMEM((others, *face), jnp.float32),
            dma((4,)), dma((2, columns // width)), dma((2, 2)), dma((others, 1 + columns // width)),
            dma, dma, dma((others,)),
            pltpu.SemaphoreType.REGULAR,
        ],
        compiler_params=pltpu.CompilerParams(
            collective_id=0, has_side_effects=True, vmem_limit_bytes=48 * 1024 * 1024),
    )(*flat)
    results = pl.pallas_call(
        functools.partial(write_out, sizes, depth),
        out_shape=(out, out),
        in_specs=[in_vmem] * len(held_shapes),
        out_specs=(pl.BlockSpec(memory_space=pltpu.HBM),) * 2,
        scratch_shapes=[last, last, dma((2,))],
        compiler_params=pltpu.CompilerParams(vmem_limit_bytes=8 * 1024 * 1024),
    )(*held)
    return tuple(array.reshape(rows, columns, depth, levels) for array in results)


def solution(mesh):
    spec = P("south", "east", "down", None)
    sizes = {axis: mesh.shape[axis] for axis in AXES}
    return jax.shard_map(
        functools.partial(local, sizes), mesh=mesh, in_specs=(spec,) * 4,
        out_specs=(spec, spec), check_vma=False)
```

```python
import functools

import jax
import jax.numpy as jnp
from jax import lax
from jax.experimental import pallas as pl
from jax.experimental.pallas import tpu as pltpu
from jax.sharding import PartitionSpec as P

STEPS = 4
AXES = ("south", "east", "down")
MESH = pl.DeviceIdType.MESH


def group_of(columns):
    return next(size for size in (8, 4, 2, 1) if columns % size == 0)


def chunk_of(columns, group):
    return next(size for size in (2 * group, group) if columns % size == 0)


def each(count, body):
    def one(i, carry):
        body(i)
        return carry

    lax.fori_loop(0, count, one, 0)


def new_values(depth, group, u, halos, fy, fx, fz, t, y, row, x0):
    levels = u.shape[-1]
    place = lax.broadcasted_iota(jnp.int32, (depth, levels), 0)

    def at(x, pad):
        return pl.ds(pl.multiple_of((x + pad) * depth, 8), depth)

    line = [u[t - 1, y + 1, at(x0 + g, 0), :] for g in range(group + 2)]
    values = []
    for g in range(group):
        x = x0 + g
        mid, west, east_of = line[g + 1], line[g], line[g + 2]
        north, south_of = u[t - 1, y, at(x, 1), :], u[t - 1, y + 2, at(x, 1), :]
        low = jnp.broadcast_to(halos[t - 1, 0, row, pl.ds(x, 1), :], (depth, levels))
        high = jnp.broadcast_to(halos[t - 1, 1, row, pl.ds(x, 1), :], (depth, levels))
        low = jnp.where(place == 0, low, pltpu.roll(mid, 1, 0))
        high = jnp.where(place == depth - 1, high, pltpu.roll(mid, depth - 1, 0))
        own = at(x, 0)
        spread = (north + south_of) + (west + east_of) + (low + high) - 6.0 * mid
        values.append(mid - fy[row, own, :] * (south_of - north) - fx[row, own, :] * (east_of - west)
                      - fz[row, own, :] * (high - low) + 0.05 * spread)
    return values


def running_sum(value):
    depth = value.shape[0]
    place = lax.broadcasted_iota(jnp.int32, value.shape, 0)
    hop = 1
    while hop < depth:
        value = value + jnp.where(place >= hop, pltpu.roll(value, hop, 0), 0.0)
        hop *= 2
    return value


def finished(sizes, totals_in, row, x, value):
    rank = lax.axis_index("down")
    for hop in range(1, sizes["down"]):
        below = jnp.broadcast_to(totals_in[hop - 1, row, pl.ds(x, 1), :], value.shape)
        value = value + jnp.where(rank >= hop, below, 0.0)
    return value * (1.0 / (value.shape[0] * sizes["down"]))


def kernel(sizes, depth, field, flow_y, flow_x, flow_z, pot, end, last_u, last_flows, last_halos, last_totals,
           u, fy, fx, fz, faces, halos, totals, totals_in, load_sem, south_recv, side_recv, tot_recv, south_send, side_send, tot_send, go):
    rows, cells, levels = field.shape
    columns = cells // depth
    group = group_of(columns)
    width = chunk_of(columns, group)
    chunks = columns // width
    places = {axis: lax.axis_index(axis) for axis in AXES}

    def beside(axis, hop):
        return {axis: lax.rem(places[axis] + hop, sizes[axis])}

    near = lax.rem(places["south"], 2)
    leads = lax.rem(places["down"], 2) == 0
    follows = jnp.logical_not(leads)
    split = sizes["down"] == 2 and sizes["south"] % 2 == 0 and sizes["south"] > 2
    hops = [(axis, hop) for axis in ("south", "east") for hop in sorted({1, sizes[axis] - 1})]
    barrier = pltpu.get_barrier_semaphore()
    partner = beside("south", 1 + near * (sizes["south"] - 2))

    def greet(device_id):
        pl.semaphore_signal(barrier, inc=1, device_id=device_id, device_id_type=MESH)

    if split:
        @pl.when(follows)
        def _():
            greet(partner)
            greet({"down": 0})

        for axis, hop in hops:
            greet({**beside(axis, hop), "down": 0})
    else:
        hops += [("down", hop) for hop in range(1, sizes["down"])]
        for axis, hop in hops:
            greet(beside(axis, hop))

    def load(src, dst, sem):
        return pltpu.make_async_copy(src, dst, load_sem.at[sem])

    def done(ref, sem):
        pltpu.make_async_copy(ref, ref, sem).wait()

    rims = [load(field.at[y], u.at[0, y + 1, pl.ds(depth, cells), :], 0) for y in (0, rows - 1)]
    inner = load(field.at[pl.ds(1, rows - 2)], u.at[0, pl.ds(2, rows - 2), pl.ds(depth, cells), :], 1)
    flows = [load(src, dst, 2) for src, dst in ((flow_y, fy), (flow_x, fx), (flow_z, fz))]
    for copy in rims:
        copy.start()

    def chunk_at(c):
        return pl.ds(pl.multiple_of(c * width * depth + depth, 8), width * depth)

    def south(t, side, c):
        return pltpu.make_async_remote_copy(
            src_ref=u.at[t, (1 - side) * (rows - 1) + 1, chunk_at(c), :],
            dst_ref=u.at[t, side * (rows + 1), chunk_at(c), :],
            send_sem=south_send, recv_sem=south_recv.at[t % 2, c],
            device_id=beside("south", 1 + side * (sizes["south"] - 2)), device_id_type=MESH)

    def south_done(t, c):
        done(u.at[t, pl.ds(0, 2), chunk_at(c), :], south_recv.at[t % 2, c])

    blocks = ((1, rows - 2), (0, 1), (rows - 1, 1))

    def east(t, side, part):
        start, count = blocks[part]
        column = columns if side == 0 else 1
        if t == 0:
            src = field.at[pl.ds(start, count), pl.ds((column - 1) * depth, depth), :]
        else:
            src = u.at[t, pl.ds(start + 1, count), pl.ds(column * depth, depth), :]
        return pltpu.make_async_remote_copy(
            src_ref=src,
            dst_ref=u.at[t, pl.ds(start + 1, count), pl.ds(0 if side == 0 else cells + depth, depth), :],
            send_sem=side_send, recv_sem=side_recv.at[t % 2, min(part, 1)],
            device_id=beside("east", 1 if side == 0 else sizes["east"] - 1), device_id_type=MESH)

    def down(t, side, part):
        start, count = blocks[part]
        return pltpu.make_async_remote_copy(
            src_ref=faces.at[t, side, pl.ds(start, count)],
            dst_ref=halos.at[t, side, pl.ds(start, count)],
            send_sem=side_send, recv_sem=side_recv.at[t % 2, min(part, 1)],
            device_id=beside("down", 1 if side == 0 else sizes["down"] - 1), device_id_type=MESH)

    def sides_start(t, parts):
        for part in parts:
            for side in (0, 1):
                down(t, side, part).start()
                east(t, side, part).start()

    both = 2 * (depth + columns)

    def sides_done(t, part):
        done(u.at[t, pl.ds(0, rows - 2 if part == 0 else 2), pl.ds(0, both), :], side_recv.at[t % 2, part])

    def total(hop, piece, y0, count, x0, span):
        cut = (pl.ds(y0, count), pl.ds(x0, span))
        return pltpu.make_async_remote_copy(
            src_ref=totals.at[cut], dst_ref=totals_in.at[(hop - 1, *cut)],
            send_sem=tot_send.at[hop - 1], recv_sem=tot_recv.at[hop - 1, piece],
            device_id=beside("down", hop), device_id_type=MESH)

    def rim_at(c):
        return pl.multiple_of(c * width, group)

    def take_faces(t, y, x0):
        for side, place in ((0, depth - 1), (1, 0)):
            start = (x0 + 1) * depth + place
            faces[t, side, y, pl.ds(x0, group), :] = u[t, y + 1, pl.ds(start, group, stride=depth), :]

    def march(t, y, x0):
        values = new_values(depth, group, u, halos, fy, fx, fz, t, y, y, x0)
        for g, value in enumerate(values):
            if t < STEPS:
                u[t, y + 1, pl.ds(pl.multiple_of((x0 + g + 1) * depth, 8), depth), :] = value
            else:
                own = pl.ds(pl.multiple_of((x0 + g) * depth, 8), depth)
                end[y, own, :] = value
                pot[y, own, :] = running_sum(value)
        if t < STEPS:
            take_faces(t, y, x0)
        else:
            start = x0 * depth + depth - 1
            totals[y, pl.ds(x0, group), :] = pot[y, pl.ds(start, group, stride=depth), :]

    def over(y0, count, x0, span, body):
        groups = span // group
        each(count * groups,
             lambda i: body(y0 + i // groups, pl.multiple_of(x0 + (i % groups) * group, group)))

    def finish(y, x0):
        for g in range(group):
            own = pl.ds(pl.multiple_of((x0 + g) * depth, 8), depth)
            pot[y, own, :] = finished(sizes, totals_in, y, x0 + g, pot[y, own, :])

    down_hops = range(1, sizes["down"])
    last_rank = sizes["down"] - 1

    def upwards(body):
        for hop in down_hops:
            pl.when(places["down"] + hop <= last_rank)(functools.partial(body, hop))

    def from_below(body):
        for hop in down_hops:
            pl.when(places["down"] >= hop)(functools.partial(body, hop))

    def rim_over(c, body):
        groups = width // group
        each(2 * groups, lambda i: body((i // groups) * (rows - 1),
                                        pl.multiple_of(c * width + (i % groups) * group, group)))

    last_block = sizes["south"] - 1
    first = jnp.where(places["south"] == last_block, 0, jnp.where(places["south"] == 1, 1, 1 - near))
    lag = min(4, chunks)

    def send_chunk(t, c):
        south(t, 1 - near, c).start()
        south(t, near, c).start()

    def send_last(c):
        south(STEPS - 1, first, c).start()
        pl.when(c >= lag)(lambda: south(STEPS - 1, 1 - first, c - lag).start())

    def send_first():
        each(chunks, lambda c: send_chunk(0, c))

    def send_far():
        each(chunks, lambda c: south(0, 1 - near, c).start())

    def send_rim_totals(c):
        def one(hop):
            for y in (0, rows - 1):
                total(hop, 1 + c, y, 1, rim_at(c), width).start()

        upwards(one)

    def take_rim_totals(c):
        from_below(lambda hop: done(totals_in.at[hop - 1, pl.ds(0, 2), pl.ds(rim_at(c), width)],
                                    tot_recv.at[hop - 1, 1 + c]))

    def finish_rim(c):
        take_rim_totals(c)
        rim_over(c, finish)

    base = columns - width
    last_cells = pl.ds(base * depth, width * depth)

    def keep_last():
        for side in (0, 1):
            row = side * (rows - 1)
            for i in (0, 1, 2):
                if (side, i) not in ((0, 0), (1, 2)):
                    last_u[0, 3 * side + i] = u[STEPS - 1, row + i, pl.ds(base * depth, (width + 2) * depth), :]
            for i, flow in enumerate((fy, fx, fz)):
                last_flows[i, side] = flow[row, last_cells, :]
            for z in (0, 1):
                last_halos[0, z, side] = halos[STEPS - 1, z, row, pl.ds(base, width), :]

    def keep_south():
        for side in (0, 1):
            last_u[0, 5 * side, pl.ds(depth, width * depth), :] = u[
                STEPS - 1, side * (rows + 1), pl.ds((base + 1) * depth, width * depth), :]

    def keep_totals():
        for hop in down_hops:
            for side in (0, 1):
                @pl.when(places["down"] >= hop)
                def _():
                    last_totals[hop - 1, side] = totals_in[hop - 1, side * (rows - 1), pl.ds(base, width), :]

                @pl.when(places["down"] < hop)
                def _():
                    last_totals[hop - 1, side] = jnp.zeros((width, levels), jnp.float32)

    if split:
        @pl.when(follows)
        def _():
            pl.semaphore_wait(barrier, 1)
            pltpu.make_async_remote_copy(
                src_ref=field.at[(1 - near) * (rows - 1), pl.ds(0, width * depth), :],
                dst_ref=u.at[0, near * (rows + 1), pl.ds(depth, width * depth), :],
                send_sem=south_send, recv_sem=south_recv.at[0, 0], device_id=partner, device_id_type=MESH).start()
    else:
        pl.semaphore_wait(barrier, len(hops))
    done(u.at[0, pl.ds(1, 2), pl.ds(depth, cells), :], load_sem.at[0])
    inner.start()
    for copy in flows:
        copy.start()
    if split:
        @pl.when(leads)
        def _():
            pl.semaphore_wait(barrier, 2 * len(hops) + 1)
            pl.semaphore_signal(go, inc=1, device_id={"down": 1}, device_id_type=MESH)

        @pl.when(follows)
        def _():
            each(chunks - 1, lambda c: south(0, near, c + 1).start())
    pl.when(leads)(send_first)
    done(u.at[0, pl.ds(2, rows - 2), pl.ds(depth, cells), :], load_sem.at[1])
    over(0, rows, 0, columns, functools.partial(take_faces, 0))
    if split:
        pl.when(follows)(lambda: pl.semaphore_wait(go, 1))
    sides_start(0, (0, 1, 2))
    if not split:
        pl.when(follows)(send_first)
    done(u.at[pl.ds(0, 3), pl.ds(0, rows), pl.ds(depth, cells), :], load_sem.at[2])

    ahead = min(3, chunks) if split else 0
    if split:
        @pl.when(leads)
        def _():
            each(ahead, lambda c: south_done(0, c))
            pl.semaphore_signal(go, inc=1, device_id={"down": 1}, device_id_type=MESH)

    def take_south(t, c):
        if t == 0 and split:
            pl.when(jnp.logical_or(follows, c >= ahead))(lambda: south_done(t, c))
        else:
            south_done(t, c)

    for t in range(1, STEPS + 1):
        sides_done(t - 1, 0)
        over(*blocks[0], 0, columns, functools.partial(march, t))
        if t == 1 and split:
            @pl.when(follows)
            def _():
                pl.semaphore_wait(go, 1)
                send_far()

        if t < STEPS:
            sides_start(t, (0,))
        else:
            upwards(lambda hop: total(hop, 0, *blocks[0], 0, columns).start())
            from_below(lambda hop: total(hop, 0, *blocks[0], 0, columns).wait_recv())
            over(*blocks[0], 0, columns, finish)
        sides_done(t - 1, 1)

        def rim(c):
            if t < STEPS:
                take_south(t - 1, c)
                rim_over(c, functools.partial(march, t))
                if t < STEPS - 1:
                    send_chunk(t, c)
                else:
                    send_last(c)
            else:
                pl.when(c > 0)(lambda: finish_rim(c - 1))
                pl.when(c == chunks - 1)(keep_last)
                take_south(t - 1, c)

                @pl.when(jnp.logical_or(c < chunks - 1, places["down"] < last_rank))
                def _():
                    rim_over(c, functools.partial(march, t))
                    send_rim_totals(c)

        each(chunks, rim)
        if t == STEPS - 1:
            each(lag, lambda c: south(t, 1 - first, chunks - lag + c).start())
        if t < STEPS:
            sides_start(t, (1, 2))
    keep_south()
    take_rim_totals(chunks - 1)
    keep_totals()
    done(u.at[:, pl.ds(0, 2), pl.ds(depth, cells), :], south_send)
    done(u.at[:, pl.ds(0, rows), pl.ds(0, both), :], side_send)
    upwards(lambda hop: done(totals, tot_send.at[hop - 1]))


def write_out(sizes, depth, pot, end, last_u, last_flows, last_halos, last_totals, pot_out, end_out,
              last_pot, last_end, sems):
    rows, cells, levels = pot.shape
    columns = cells // depth
    group = group_of(columns)
    width = chunk_of(columns, group)
    kept = cells - width * depth
    whole = ((pot, pot_out), (end, end_out))
    for i, (src, dst) in enumerate(whole):
        for y in range(1, rows - 1):
            pltpu.make_async_copy(src.at[y], dst.at[y], sems.at[i]).start()
        if kept:
            for y in (0, rows - 1):
                cut = (y, pl.ds(0, kept))
                pltpu.make_async_copy(src.at[cut], dst.at[cut], sems.at[i]).start()
    groups = width // group

    def last(i):
        side, x0 = i // groups, pl.multiple_of((i % groups) * group, group)
        values = new_values(depth, group, last_u, last_halos, *(last_flows.at[k] for k in (0, 1, 2)), 1, 3 * side, side, x0)
        for g, value in enumerate(values):
            own = pl.ds(pl.multiple_of((x0 + g) * depth, 8), depth)
            last_end[side, own, :] = value
            last_pot[side, own, :] = finished(sizes, last_totals, side, x0 + g, running_sum(value))

    each(2 * groups, last)
    for i, (src, (_, dst)) in enumerate(zip((last_pot, last_end), whole)):
        for side, y in ((0, 0), (1, rows - 1)):
            cut = (y, pl.ds(kept, cells - kept))
            pltpu.make_async_copy(src.at[side], dst.at[cut], sems.at[i]).start()
    for i, (src, dst) in enumerate(whole):
        pltpu.make_async_copy(src, dst, sems.at[i]).wait()


def local(sizes, field_values, *flows):
    rows, columns, depth, levels = field_values.shape
    cells = columns * depth
    width = chunk_of(columns, group_of(columns))
    flat = [array.reshape(rows, cells, levels) for array in (field_values, *flows)]
    block = pltpu.VMEM((rows, cells, levels), jnp.float32)
    dma = pltpu.SemaphoreType.DMA
    others = sizes["down"] - 1
    face = (rows, columns, levels)
    out = jax.ShapeDtypeStruct((rows, cells, levels), jnp.float32)
    in_vmem = pl.BlockSpec(memory_space=pltpu.VMEM)
    last = pltpu.VMEM((2, width * depth, levels), jnp.float32)
    held_shapes = (
        block, block,
        pltpu.VMEM((1, 6, (width + 2) * depth, levels), jnp.float32),
        pltpu.VMEM((3, 2, width * depth, levels), jnp.float32),
        pltpu.VMEM((1, 2, 2, width, levels), jnp.float32),
        pltpu.VMEM((others, 2, width, levels), jnp.float32),
    )
    held = pl.pallas_call(
        functools.partial(kernel, sizes, depth),
        out_shape=held_shapes,
        in_specs=[pl.BlockSpec(memory_space=pl.ANY)] * 4,
        out_specs=(in_vmem,) * len(held_shapes),
        scratch_shapes=[
            pltpu.VMEM((STEPS, rows + 2, cells + 2 * depth, levels), jnp.float32),
            block, block, block,
            pltpu.VMEM((STEPS, 2, *face), jnp.float32),
            pltpu.VMEM((STEPS, 2, *face), jnp.float32),
            pltpu.VMEM(face, jnp.float32),
            pltpu.VMEM((others, *face), jnp.float32),
            dma((3,)), dma((2, columns // width)), dma((2, 2)), dma((others, 1 + columns // width)),
            dma, dma, dma((others,)),
            pltpu.SemaphoreType.REGULAR,
        ],
        compiler_params=pltpu.CompilerParams(
            collective_id=0, has_side_effects=True, vmem_limit_bytes=48 * 1024 * 1024),
    )(*flat)
    results = pl.pallas_call(
        functools.partial(write_out, sizes, depth),
        out_shape=(out, out),
        in_specs=[in_vmem] * len(held_shapes),
        out_specs=(pl.BlockSpec(memory_space=pltpu.HBM),) * 2,
        scratch_shapes=[last, last, dma((2,))],
        compiler_params=pltpu.CompilerParams(vmem_limit_bytes=8 * 1024 * 1024),
    )(*held)
    return tuple(array.reshape(rows, columns, depth, levels) for array in results)


def solution(mesh):
    spec = P("south", "east", "down", None)
    sizes = {axis: mesh.shape[axis] for axis in AXES}
    return jax.shard_map(
        functools.partial(local, sizes), mesh=mesh, in_specs=(spec,) * 4,
        out_specs=(spec, spec), check_vma=False)
```

```python
import functools

import jax
import jax.numpy as jnp
from jax import lax
from jax.experimental import pallas as pl
from jax.experimental.pallas import tpu as pltpu
from jax.sharding import PartitionSpec as P

STEPS = 4
AXES = ("south", "east", "down")
MESH = pl.DeviceIdType.MESH


def group_of(columns):
    return next(size for size in (8, 4, 2, 1) if columns % size == 0)


def chunk_of(columns, group):
    return next(size for size in (2 * group, group) if columns % size == 0)


def each(count, body):
    def one(i, carry):
        body(i)
        return carry

    lax.fori_loop(0, count, one, 0)


def new_values(depth, group, u, halos, fy, fx, fz, t, y, row, x0):
    levels = u.shape[-1]
    place = lax.broadcasted_iota(jnp.int32, (depth, levels), 0)

    def at(x, pad):
        return pl.ds(pl.multiple_of((x + pad) * depth, 8), depth)

    line = [u[t - 1, y + 1, at(x0 + g, 0), :] for g in range(group + 2)]
    values = []
    for g in range(group):
        x = x0 + g
        mid, west, east_of = line[g + 1], line[g], line[g + 2]
        north, south_of = u[t - 1, y, at(x, 1), :], u[t - 1, y + 2, at(x, 1), :]
        low = jnp.broadcast_to(halos[t - 1, 0, row, pl.ds(x, 1), :], (depth, levels))
        high = jnp.broadcast_to(halos[t - 1, 1, row, pl.ds(x, 1), :], (depth, levels))
        low = jnp.where(place == 0, low, pltpu.roll(mid, 1, 0))
        high = jnp.where(place == depth - 1, high, pltpu.roll(mid, depth - 1, 0))
        own = at(x, 0)
        spread = (north + south_of) + (west + east_of) + (low + high) - 6.0 * mid
        values.append(mid - fy[row, own, :] * (south_of - north) - fx[row, own, :] * (east_of - west)
                      - fz[row, own, :] * (high - low) + 0.05 * spread)
    return values


def running_sum(value):
    depth = value.shape[0]
    place = lax.broadcasted_iota(jnp.int32, value.shape, 0)
    hop = 1
    while hop < depth:
        value = value + jnp.where(place >= hop, pltpu.roll(value, hop, 0), 0.0)
        hop *= 2
    return value


def finished(sizes, totals_in, row, x, value):
    rank = lax.axis_index("down")
    for hop in range(1, sizes["down"]):
        below = jnp.broadcast_to(totals_in[hop - 1, row, pl.ds(x, 1), :], value.shape)
        value = value + jnp.where(rank >= hop, below, 0.0)
    return value * (1.0 / (value.shape[0] * sizes["down"]))


def kernel(sizes, depth, field, flow_y, flow_x, flow_z, pot, end, last_u, last_flows, last_halos, totals_in,
           u, fy, fx, fz, faces, halos, totals, load_sem, south_recv, side_recv, tot_recv, south_send, side_send, tot_send, go):
    rows, cells, levels = field.shape
    columns = cells // depth
    group = group_of(columns)
    width = chunk_of(columns, group)
    chunks = columns // width
    places = {axis: lax.axis_index(axis) for axis in AXES}

    def beside(axis, hop):
        return {axis: lax.rem(places[axis] + hop, sizes[axis])}

    near = lax.rem(places["south"], 2)
    leads = lax.rem(places["down"], 2) == 0
    follows = jnp.logical_not(leads)
    split = sizes["down"] == 2 and sizes["south"] % 2 == 0 and sizes["south"] > 2
    hops = [(axis, hop) for axis in ("south", "east") for hop in sorted({1, sizes[axis] - 1})]
    barrier = pltpu.get_barrier_semaphore()
    partner = beside("south", 1 + near * (sizes["south"] - 2))

    def greet(device_id):
        pl.semaphore_signal(barrier, inc=1, device_id=device_id, device_id_type=MESH)

    if split:
        @pl.when(follows)
        def _():
            greet(partner)
            greet({"down": 0})

        for axis, hop in hops:
            greet({**beside(axis, hop), "down": 0})
    else:
        hops += [("down", hop) for hop in range(1, sizes["down"])]
        for axis, hop in hops:
            greet(beside(axis, hop))

    def load(src, dst, sem):
        return pltpu.make_async_copy(src, dst, load_sem.at[sem])

    def done(ref, sem):
        pltpu.make_async_copy(ref, ref, sem).wait()

    rims = [load(field.at[y], u.at[0, y + 1, pl.ds(depth, cells), :], 0) for y in (0, rows - 1)]
    inner = load(field.at[pl.ds(1, rows - 2)], u.at[0, pl.ds(2, rows - 2), pl.ds(depth, cells), :], 1)
    flows = [load(src, dst, 2) for src, dst in ((flow_y, fy), (flow_x, fx), (flow_z, fz))]
    for copy in rims:
        copy.start()

    def chunk_at(c):
        return pl.ds(pl.multiple_of(c * width * depth + depth, 8), width * depth)

    def south(t, side, c):
        return pltpu.make_async_remote_copy(
            src_ref=u.at[t, (1 - side) * (rows - 1) + 1, chunk_at(c), :],
            dst_ref=u.at[t, side * (rows + 1), chunk_at(c), :],
            send_sem=south_send, recv_sem=south_recv.at[t % 2, c],
            device_id=beside("south", 1 + side * (sizes["south"] - 2)), device_id_type=MESH)

    def south_done(t, c):
        done(u.at[t, pl.ds(0, 2), chunk_at(c), :], south_recv.at[t % 2, c])

    blocks = ((1, rows - 2), (0, 1), (rows - 1, 1))

    def east(t, side, part):
        start, count = blocks[part]
        column = columns if side == 0 else 1
        if t == 0:
            src = field.at[pl.ds(start, count), pl.ds((column - 1) * depth, depth), :]
        else:
            src = u.at[t, pl.ds(start + 1, count), pl.ds(column * depth, depth), :]
        return pltpu.make_async_remote_copy(
            src_ref=src,
            dst_ref=u.at[t, pl.ds(start + 1, count), pl.ds(0 if side == 0 else cells + depth, depth), :],
            send_sem=side_send, recv_sem=side_recv.at[t % 2, min(part, 1)],
            device_id=beside("east", 1 if side == 0 else sizes["east"] - 1), device_id_type=MESH)

    def down(t, side, part):
        start, count = blocks[part]
        return pltpu.make_async_remote_copy(
            src_ref=faces.at[t, side, pl.ds(start, count)],
            dst_ref=halos.at[t, side, pl.ds(start, count)],
            send_sem=side_send, recv_sem=side_recv.at[t % 2, min(part, 1)],
            device_id=beside("down", 1 if side == 0 else sizes["down"] - 1), device_id_type=MESH)

    def sides_start(t, parts):
        for part in parts:
            for side in (0, 1):
                down(t, side, part).start()
                east(t, side, part).start()

    both = 2 * (depth + columns)

    def sides_done(t, part):
        done(u.at[t, pl.ds(0, rows - 2 if part == 0 else 2), pl.ds(0, both), :], side_recv.at[t % 2, part])

    def total(hop, piece, y0, count, x0, span):
        cut = (pl.ds(y0, count), pl.ds(x0, span))
        return pltpu.make_async_remote_copy(
            src_ref=totals.at[cut], dst_ref=totals_in.at[(hop - 1, *cut)],
            send_sem=tot_send.at[hop - 1], recv_sem=tot_recv.at[hop - 1, piece],
            device_id=beside("down", hop), device_id_type=MESH)

    def rim_at(c):
        return pl.multiple_of(c * width, group)

    def take_faces(t, y, x0):
        for side, place in ((0, depth - 1), (1, 0)):
            start = (x0 + 1) * depth + place
            faces[t, side, y, pl.ds(x0, group), :] = u[t, y + 1, pl.ds(start, group, stride=depth), :]

    def march(t, y, x0):
        values = new_values(depth, group, u, halos, fy, fx, fz, t, y, y, x0)
        for g, value in enumerate(values):
            if t < STEPS:
                u[t, y + 1, pl.ds(pl.multiple_of((x0 + g + 1) * depth, 8), depth), :] = value
            else:
                own = pl.ds(pl.multiple_of((x0 + g) * depth, 8), depth)
                end[y, own, :] = value
                pot[y, own, :] = running_sum(value)
        if t < STEPS:
            take_faces(t, y, x0)
        else:
            start = x0 * depth + depth - 1
            totals[y, pl.ds(x0, group), :] = pot[y, pl.ds(start, group, stride=depth), :]

    def over(y0, count, x0, span, body):
        groups = span // group
        each(count * groups,
             lambda i: body(y0 + i // groups, pl.multiple_of(x0 + (i % groups) * group, group)))

    def finish(y, x0):
        for g in range(group):
            own = pl.ds(pl.multiple_of((x0 + g) * depth, 8), depth)
            pot[y, own, :] = finished(sizes, totals_in, y, x0 + g, pot[y, own, :])

    down_hops = range(1, sizes["down"])
    last_rank = sizes["down"] - 1

    def upwards(body):
        for hop in down_hops:
            pl.when(places["down"] + hop <= last_rank)(functools.partial(body, hop))

    def from_below(body):
        for hop in down_hops:
            pl.when(places["down"] >= hop)(functools.partial(body, hop))

    def rim_over(c, body):
        groups = width // group
        each(2 * groups, lambda i: body((i // groups) * (rows - 1),
                                        pl.multiple_of(c * width + (i % groups) * group, group)))

    last_block = sizes["south"] - 1
    first = jnp.where(places["south"] == last_block, 0, jnp.where(places["south"] == 1, 1, 1 - near))
    lag = min(4, chunks)

    def send_chunk(t, c):
        south(t, 1 - near, c).start()
        south(t, near, c).start()

    def send_last(c):
        south(STEPS - 1, first, c).start()
        pl.when(c >= lag)(lambda: south(STEPS - 1, 1 - first, c - lag).start())

    def send_first():
        each(chunks, lambda c: send_chunk(0, c))

    def send_far():
        each(chunks, lambda c: south(0, 1 - near, c).start())

    def send_rim_totals(c):
        def one(hop):
            for y in (0, rows - 1):
                total(hop, 1, y, 1, rim_at(c), width).start()

        upwards(one)

    def take_rim_totals():
        from_below(lambda hop: done(totals_in.at[hop - 1, pl.ds(0, 2)], tot_recv.at[hop - 1, 1]))

    base = columns - width
    last_cells = pl.ds(base * depth, width * depth)

    def keep_last():
        for side in (0, 1):
            row = side * (rows - 1)
            for i in (0, 1, 2):
                if (side, i) not in ((0, 0), (1, 2)):
                    last_u[0, 3 * side + i] = u[STEPS - 1, row + i, pl.ds(base * depth, (width + 2) * depth), :]
            for i, flow in enumerate((fy, fx, fz)):
                last_flows[i, side] = flow[row, last_cells, :]
            for z in (0, 1):
                last_halos[0, z, side] = halos[STEPS - 1, z, row, pl.ds(base, width), :]

    def keep_south():
        for side in (0, 1):
            last_u[0, 5 * side, pl.ds(depth, width * depth), :] = u[
                STEPS - 1, side * (rows + 1), pl.ds((base + 1) * depth, width * depth), :]

    if split:
        @pl.when(jnp.logical_and(follows, near == 1))
        def _():
            pl.semaphore_wait(barrier, 1)
            pltpu.make_async_remote_copy(
                src_ref=field.at[(1 - near) * (rows - 1), pl.ds(0, width * depth), :],
                dst_ref=u.at[0, near * (rows + 1), pl.ds(depth, width * depth), :],
                send_sem=south_send, recv_sem=south_recv.at[0, 0], device_id=partner, device_id_type=MESH).start()
    else:
        pl.semaphore_wait(barrier, len(hops))
    done(u.at[0, pl.ds(1, 2), pl.ds(depth, cells), :], load_sem.at[0])
    inner.start()
    for copy in flows:
        copy.start()
    if split:
        @pl.when(leads)
        def _():
            pl.semaphore_wait(barrier, 2 * len(hops) + 1)
            pl.semaphore_signal(go, inc=1, device_id={"down": 1}, device_id_type=MESH)

        @pl.when(jnp.logical_and(follows, near == 0))
        def _():
            pl.semaphore_wait(barrier, 1)
            south(0, near, 0).start()

        @pl.when(follows)
        def _():
            each(chunks - 1, lambda c: south(0, near, c + 1).start())
    pl.when(leads)(send_first)
    done(u.at[0, pl.ds(2, rows - 2), pl.ds(depth, cells), :], load_sem.at[1])
    over(0, rows, 0, columns, functools.partial(take_faces, 0))
    if split:
        pl.when(follows)(lambda: pl.semaphore_wait(go, 1))
    sides_start(0, (0, 1, 2))
    if not split:
        pl.when(follows)(send_first)
    done(u.at[pl.ds(0, 3), pl.ds(0, rows), pl.ds(depth, cells), :], load_sem.at[2])

    ahead = min(3, chunks) if split else 0

    def let_go():
        @pl.when(leads)
        def _():
            each(ahead, lambda c: south_done(0, c))
            pl.semaphore_signal(go, inc=1, device_id={"down": 1}, device_id_type=MESH)

        @pl.when(follows)
        def _():
            pl.semaphore_wait(go, 1)
            send_far()

    def take_south(t, c):
        if t == 0 and split:
            pl.when(jnp.logical_or(follows, c >= ahead))(lambda: south_done(t, c))
        else:
            south_done(t, c)

    for t in range(1, STEPS + 1):
        sides_done(t - 1, 0)
        if t == 1 and split:
            half = (rows - 2) // 2
            over(1, half, 0, columns, functools.partial(march, t))
            let_go()
            over(1 + half, rows - 2 - half, 0, columns, functools.partial(march, t))
        else:
            over(*blocks[0], 0, columns, functools.partial(march, t))
        if t < STEPS:
            sides_start(t, (0,))
        else:
            upwards(lambda hop: total(hop, 0, *blocks[0], 0, columns).start())
            from_below(lambda hop: total(hop, 0, *blocks[0], 0, columns).wait_recv())
            over(*blocks[0], 0, columns, finish)
        sides_done(t - 1, 1)

        def rim(c):
            if t < STEPS:
                take_south(t - 1, c)
                rim_over(c, functools.partial(march, t))
                if t < STEPS - 1:
                    send_chunk(t, c)
                else:
                    send_last(c)
            else:
                pl.when(c == chunks - 1)(keep_last)
                take_south(t - 1, c)

                @pl.when(jnp.logical_or(c < chunks - 1, places["down"] < last_rank))
                def _():
                    rim_over(c, functools.partial(march, t))
                    send_rim_totals(c)

        each(chunks, rim)
        if t == STEPS - 1:
            each(lag, lambda c: south(t, 1 - first, chunks - lag + c).start())
        if t < STEPS:
            sides_start(t, (1, 2))
    keep_south()
    take_rim_totals()
    done(u.at[:, pl.ds(0, 2), pl.ds(depth, cells), :], south_send)
    done(u.at[:, pl.ds(0, rows), pl.ds(0, both), :], side_send)
    upwards(lambda hop: done(totals, tot_send.at[hop - 1]))


def write_out(sizes, depth, pot, end, last_u, last_flows, last_halos, totals_in, pot_out, end_out,
              rim_pot, last_end, sems):
    rows, cells, levels = pot.shape
    columns = cells // depth
    group = group_of(columns)
    width = chunk_of(columns, group)
    base = columns - width
    kept = base * depth
    sides = ((0, 0), (1, rows - 1))

    def write(i, src, dst):
        pltpu.make_async_copy(src, dst, sems.at[i]).start()

    for i, (src, dst) in enumerate(((pot, pot_out), (end, end_out))):
        for y in range(1, rows - 1):
            write(i, src.at[y], dst.at[y])
    if kept:
        for _, y in sides:
            write(1, end.at[y, pl.ds(0, kept)], end_out.at[y, pl.ds(0, kept)])

    def at(x):
        return pl.ds(pl.multiple_of(x * depth, 8), depth)

    def last(i):
        side, x0 = i % 2, pl.multiple_of((i // 2) * group, group)
        flows = [last_flows.at[k] for k in (0, 1, 2)]
        values = new_values(depth, group, last_u, last_halos, *flows, 1, 3 * side, side, x0)
        for g, value in enumerate(values):
            last_end[side, at(x0 + g), :] = value
            x = base + x0 + g
            rim_pot[side, at(x), :] = finished(sizes, totals_in, side * (rows - 1), x, running_sum(value))

    def before(i):
        side, x0 = i % 2, pl.multiple_of((i // 2) * group, group)
        y = side * (rows - 1)
        for g in range(group):
            rim_pot[side, at(x0 + g), :] = finished(sizes, totals_in, y, x0 + g, pot[y, at(x0 + g), :])

    each(2 * (base // group), before)
    each(2 * (width // group), last)
    for side, y in sides:
        write(0, rim_pot.at[side], pot_out.at[y])
        write(1, last_end.at[side], end_out.at[y, pl.ds(kept, cells - kept)])
    pltpu.make_async_copy(pot, pot_out, sems.at[0]).wait()
    pltpu.make_async_copy(end, end_out, sems.at[1]).wait()


def local(sizes, field_values, *flows):
    rows, columns, depth, levels = field_values.shape
    cells = columns * depth
    width = chunk_of(columns, group_of(columns))
    flat = [array.reshape(rows, cells, levels) for array in (field_values, *flows)]
    block = pltpu.VMEM((rows, cells, levels), jnp.float32)
    dma = pltpu.SemaphoreType.DMA
    others = sizes["down"] - 1
    face = (rows, columns, levels)
    out = jax.ShapeDtypeStruct((rows, cells, levels), jnp.float32)
    in_vmem = pl.BlockSpec(memory_space=pltpu.VMEM)
    last = pltpu.VMEM((2, width * depth, levels), jnp.float32)
    held_shapes = (
        block, block,
        pltpu.VMEM((1, 6, (width + 2) * depth, levels), jnp.float32),
        pltpu.VMEM((3, 2, width * depth, levels), jnp.float32),
        pltpu.VMEM((1, 2, 2, width, levels), jnp.float32),
        pltpu.VMEM((others, *face), jnp.float32),
    )
    held = pl.pallas_call(
        functools.partial(kernel, sizes, depth),
        out_shape=held_shapes,
        in_specs=[pl.BlockSpec(memory_space=pl.ANY)] * 4,
        out_specs=(in_vmem,) * len(held_shapes),
        scratch_shapes=[
            pltpu.VMEM((STEPS, rows + 2, cells + 2 * depth, levels), jnp.float32),
            block, block, block,
            pltpu.VMEM((STEPS, 2, *face), jnp.float32),
            pltpu.VMEM((STEPS, 2, *face), jnp.float32),
            pltpu.VMEM(face, jnp.float32),
            dma((3,)), dma((2, columns // width)), dma((2, 2)), dma((others, 2)),
            dma, dma, dma((others,)),
            pltpu.SemaphoreType.REGULAR,
        ],
        compiler_params=pltpu.CompilerParams(
            collective_id=0, has_side_effects=True, vmem_limit_bytes=48 * 1024 * 1024),
    )(*flat)
    results = pl.pallas_call(
        functools.partial(write_out, sizes, depth),
        out_shape=(out, out),
        in_specs=[in_vmem] * len(held_shapes),
        out_specs=(pl.BlockSpec(memory_space=pltpu.HBM),) * 2,
        scratch_shapes=[pltpu.VMEM((2, cells, levels), jnp.float32), last, dma((2,))],
        compiler_params=pltpu.CompilerParams(vmem_limit_bytes=8 * 1024 * 1024),
    )(*held)
    return tuple(array.reshape(rows, columns, depth, levels) for array in results)


def solution(mesh):
    spec = P("south", "east", "down", None)
    sizes = {axis: mesh.shape[axis] for axis in AXES}
    return jax.shard_map(
        functools.partial(local, sizes), mesh=mesh, in_specs=(spec,) * 4,
        out_specs=(spec, spec), check_vma=False)
```

```python
import functools

import jax
import jax.numpy as jnp
from jax import lax
from jax.experimental import pallas as pl
from jax.experimental.pallas import tpu as pltpu
from jax.sharding import PartitionSpec as P

STEPS = 4
AXES = ("south", "east", "down")
MESH = pl.DeviceIdType.MESH


def group_of(columns):
    return next(size for size in (8, 4, 2, 1) if columns % size == 0)


def chunk_of(columns, group):
    return next(size for size in (2 * group, group) if columns % size == 0)


def each(count, body):
    def one(i, carry):
        body(i)
        return carry

    lax.fori_loop(0, count, one, 0)


def new_values(depth, group, u, halos, fy, fx, fz, t, y, row, x0):
    levels = u.shape[-1]
    place = lax.broadcasted_iota(jnp.int32, (depth, levels), 0)

    def at(x, pad):
        return pl.ds(pl.multiple_of((x + pad) * depth, 8), depth)

    line = [u[t - 1, y + 1, at(x0 + g, 0), :] for g in range(group + 2)]
    values = []
    for g in range(group):
        x = x0 + g
        mid, west, east_of = line[g + 1], line[g], line[g + 2]
        north, south_of = u[t - 1, y, at(x, 1), :], u[t - 1, y + 2, at(x, 1), :]
        low = jnp.broadcast_to(halos[t - 1, 0, row, pl.ds(x, 1), :], (depth, levels))
        high = jnp.broadcast_to(halos[t - 1, 1, row, pl.ds(x, 1), :], (depth, levels))
        low = jnp.where(place == 0, low, pltpu.roll(mid, 1, 0))
        high = jnp.where(place == depth - 1, high, pltpu.roll(mid, depth - 1, 0))
        own = at(x, 0)
        spread = (north + south_of) + (west + east_of) + (low + high) - 6.0 * mid
        values.append(mid - fy[row, own, :] * (south_of - north) - fx[row, own, :] * (east_of - west)
                      - fz[row, own, :] * (high - low) + 0.05 * spread)
    return values


def running_sum(value):
    depth = value.shape[0]
    place = lax.broadcasted_iota(jnp.int32, value.shape, 0)
    hop = 1
    while hop < depth:
        value = value + jnp.where(place >= hop, pltpu.roll(value, hop, 0), 0.0)
        hop *= 2
    return value


def finished(sizes, totals_in, row, x, value):
    rank = lax.axis_index("down")
    for hop in range(1, sizes["down"]):
        below = jnp.broadcast_to(totals_in[hop - 1, row, pl.ds(x, 1), :], value.shape)
        value = value + jnp.where(rank >= hop, below, 0.0)
    return value * (1.0 / (value.shape[0] * sizes["down"]))


def kernel(sizes, depth, field, flow_y, flow_x, flow_z, pot, end, last_u, last_flows, last_halos, totals_in,
           u, fy, fx, fz, faces, halos, totals, south_recv, side_recv, tot_recv, south_send, side_send, tot_send, go):
    rows, cells, levels = field.shape
    columns = cells // depth
    group = group_of(columns)
    width = chunk_of(columns, group)
    chunks = columns // width
    places = {axis: lax.axis_index(axis) for axis in AXES}

    def beside(axis, hop):
        return {axis: lax.rem(places[axis] + hop, sizes[axis])}

    near = lax.rem(places["south"], 2)
    leads = lax.rem(places["down"], 2) == 0
    follows = jnp.logical_not(leads)
    split = sizes["down"] == 2 and sizes["south"] % 2 == 0 and sizes["south"] > 2
    hops = [(axis, hop) for axis in ("south", "east") for hop in sorted({1, sizes[axis] - 1})]
    barrier = pltpu.get_barrier_semaphore()
    partner = beside("south", 1 + near * (sizes["south"] - 2))

    def greet(device_id):
        pl.semaphore_signal(barrier, inc=1, device_id=device_id, device_id_type=MESH)

    if split:
        @pl.when(follows)
        def _():
            greet(partner)
            greet({"down": 0})

        for axis, hop in hops:
            greet({**beside(axis, hop), "down": 0})
    else:
        hops += [("down", hop) for hop in range(1, sizes["down"])]
        for axis, hop in hops:
            greet(beside(axis, hop))

    def load(src, dst, sem):
        return pltpu.make_async_copy(src, dst, sem)

    def done(ref, sem):
        pltpu.make_async_copy(ref, ref, sem).wait()

    rims_sem, inner_sem, flows_sem = side_recv.at[1, 0], side_recv.at[1, 1], tot_recv.at[0, 0]
    rims = [load(field.at[y], u.at[0, y + 1, pl.ds(depth, cells), :], rims_sem) for y in (0, rows - 1)]
    inner = load(field.at[pl.ds(1, rows - 2)], u.at[0, pl.ds(2, rows - 2), pl.ds(depth, cells), :], inner_sem)
    flows = [load(src, dst, flows_sem) for src, dst in ((flow_y, fy), (flow_x, fx), (flow_z, fz))]
    for copy in rims:
        copy.start()

    def chunk_at(c):
        return pl.ds(pl.multiple_of(c * width * depth + depth, 8), width * depth)

    def south(t, side, c):
        return pltpu.make_async_remote_copy(
            src_ref=u.at[t, (1 - side) * (rows - 1) + 1, chunk_at(c), :],
            dst_ref=u.at[t, side * (rows + 1), chunk_at(c), :],
            send_sem=south_send, recv_sem=south_recv.at[t % 2, c],
            device_id=beside("south", 1 + side * (sizes["south"] - 2)), device_id_type=MESH)

    def south_done(t, c):
        done(u.at[t, pl.ds(0, 2), chunk_at(c), :], south_recv.at[t % 2, c])

    blocks = ((1, rows - 2), (0, 1), (rows - 1, 1))

    def east(t, side, part):
        start, count = blocks[part]
        column = columns if side == 0 else 1
        if t == 0:
            src = field.at[pl.ds(start, count), pl.ds((column - 1) * depth, depth), :]
        else:
            src = u.at[t, pl.ds(start + 1, count), pl.ds(column * depth, depth), :]
        return pltpu.make_async_remote_copy(
            src_ref=src,
            dst_ref=u.at[t, pl.ds(start + 1, count), pl.ds(0 if side == 0 else cells + depth, depth), :],
            send_sem=side_send, recv_sem=side_recv.at[t % 2, min(part, 1)],
            device_id=beside("east", 1 if side == 0 else sizes["east"] - 1), device_id_type=MESH)

    def down(t, side, part):
        start, count = blocks[part]
        return pltpu.make_async_remote_copy(
            src_ref=faces.at[t, side, pl.ds(start, count)],
            dst_ref=halos.at[t, side, pl.ds(start, count)],
            send_sem=side_send, recv_sem=side_recv.at[t % 2, min(part, 1)],
            device_id=beside("down", 1 if side == 0 else sizes["down"] - 1), device_id_type=MESH)

    def sides_start(t, parts):
        for part in parts:
            for side in (0, 1):
                down(t, side, part).start()
                east(t, side, part).start()

    both = 2 * (depth + columns)

    def sides_done(t, part):
        done(u.at[t, pl.ds(0, rows - 2 if part == 0 else 2), pl.ds(0, both), :], side_recv.at[t % 2, part])

    def total(hop, piece, y0, count, x0, span):
        cut = (pl.ds(y0, count), pl.ds(x0, span))
        return pltpu.make_async_remote_copy(
            src_ref=totals.at[cut], dst_ref=totals_in.at[(hop - 1, *cut)],
            send_sem=tot_send.at[hop - 1], recv_sem=tot_recv.at[hop - 1, piece],
            device_id=beside("down", hop), device_id_type=MESH)

    def rim_at(c):
        return pl.multiple_of(c * width, group)

    def take_faces(t, y, x0):
        for side, place in ((0, depth - 1), (1, 0)):
            start = (x0 + 1) * depth + place
            faces[t, side, y, pl.ds(x0, group), :] = u[t, y + 1, pl.ds(start, group, stride=depth), :]

    def march(t, y, x0):
        values = new_values(depth, group, u, halos, fy, fx, fz, t, y, y, x0)
        for g, value in enumerate(values):
            if t < STEPS:
                u[t, y + 1, pl.ds(pl.multiple_of((x0 + g + 1) * depth, 8), depth), :] = value
            else:
                own = pl.ds(pl.multiple_of((x0 + g) * depth, 8), depth)
                end[y, own, :] = value
                pot[y, own, :] = running_sum(value)
        if t < STEPS:
            take_faces(t, y, x0)
        else:
            start = x0 * depth + depth - 1
            totals[y, pl.ds(x0, group), :] = pot[y, pl.ds(start, group, stride=depth), :]

    def over(y0, count, x0, span, body):
        groups = span // group
        each(count * groups,
             lambda i: body(y0 + i // groups, pl.multiple_of(x0 + (i % groups) * group, group)))

    def finish(y, x0):
        for g in range(group):
            own = pl.ds(pl.multiple_of((x0 + g) * depth, 8), depth)
            pot[y, own, :] = finished(sizes, totals_in, y, x0 + g, pot[y, own, :])

    down_hops = range(1, sizes["down"])
    last_rank = sizes["down"] - 1

    def upwards(body):
        for hop in down_hops:
            pl.when(places["down"] + hop <= last_rank)(functools.partial(body, hop))

    def from_below(body):
        for hop in down_hops:
            pl.when(places["down"] >= hop)(functools.partial(body, hop))

    def rim_over(c, body):
        groups = width // group
        each(2 * groups, lambda i: body((i // groups) * (rows - 1),
                                        pl.multiple_of(c * width + (i % groups) * group, group)))

    last_block = sizes["south"] - 1
    first = jnp.where(places["south"] == last_block, 0, jnp.where(places["south"] == 1, 1, 1 - near))
    lag = min(4, chunks)

    def send_chunk(t, c):
        south(t, 1 - near, c).start()
        south(t, near, c).start()

    def send_last(c):
        south(STEPS - 1, first, c).start()
        pl.when(c >= lag)(lambda: south(STEPS - 1, 1 - first, c - lag).start())

    def send_first():
        each(chunks, lambda c: send_chunk(0, c))

    def send_far():
        each(chunks, lambda c: south(0, 1 - near, c).start())

    def send_rim_totals(c):
        def one(hop):
            for y in (0, rows - 1):
                total(hop, 1, y, 1, rim_at(c), width).start()

        upwards(one)

    def take_rim_totals():
        from_below(lambda hop: done(totals_in.at[hop - 1, pl.ds(0, 2)], tot_recv.at[hop - 1, 1]))

    base = columns - width
    last_cells = pl.ds(base * depth, width * depth)

    def keep_last():
        for side in (0, 1):
            row = side * (rows - 1)
            for i in (0, 1, 2):
                if (side, i) not in ((0, 0), (1, 2)):
                    last_u[0, 3 * side + i] = u[STEPS - 1, row + i, pl.ds(base * depth, (width + 2) * depth), :]
            for i, flow in enumerate((fy, fx, fz)):
                last_flows[i, side] = flow[row, last_cells, :]
            for z in (0, 1):
                last_halos[0, z, side] = halos[STEPS - 1, z, row, pl.ds(base, width), :]

    def keep_south():
        for side in (0, 1):
            last_u[0, 5 * side, pl.ds(depth, width * depth), :] = u[
                STEPS - 1, side * (rows + 1), pl.ds((base + 1) * depth, width * depth), :]

    if split:
        @pl.when(jnp.logical_and(follows, near == 1))
        def _():
            pl.semaphore_wait(barrier, 1)
            pltpu.make_async_remote_copy(
                src_ref=field.at[(1 - near) * (rows - 1), pl.ds(0, width * depth), :],
                dst_ref=u.at[0, near * (rows + 1), pl.ds(depth, width * depth), :],
                send_sem=south_send, recv_sem=south_recv.at[0, 0], device_id=partner, device_id_type=MESH).start()
    else:
        pl.semaphore_wait(barrier, len(hops))
    done(u.at[0, pl.ds(1, 2), pl.ds(depth, cells), :], rims_sem)
    inner.start()
    for copy in flows:
        copy.start()
    if split:
        @pl.when(leads)
        def _():
            pl.semaphore_wait(barrier, 2 * len(hops) + 1)
            pl.semaphore_signal(go, inc=1, device_id={"down": 1}, device_id_type=MESH)

        @pl.when(jnp.logical_and(follows, near == 0))
        def _():
            pl.semaphore_wait(barrier, 1)
            south(0, near, 0).start()

        @pl.when(follows)
        def _():
            each(chunks - 1, lambda c: south(0, near, c + 1).start())
    pl.when(leads)(send_first)
    done(u.at[0, pl.ds(2, rows - 2), pl.ds(depth, cells), :], inner_sem)
    over(0, rows, 0, columns, functools.partial(take_faces, 0))
    if split:
        pl.when(follows)(lambda: pl.semaphore_wait(go, 1))
    sides_start(0, (0, 1, 2))
    if not split:
        pl.when(follows)(send_first)
    done(u.at[pl.ds(0, 3), pl.ds(0, rows), pl.ds(depth, cells), :], flows_sem)

    ahead = min(3, chunks) if split else 0

    def let_go():
        @pl.when(leads)
        def _():
            each(ahead, lambda c: south_done(0, c))
            pl.semaphore_signal(go, inc=1, device_id={"down": 1}, device_id_type=MESH)

        @pl.when(follows)
        def _():
            pl.semaphore_wait(go, 1)
            send_far()

    def take_south(t, c):
        if t == 0 and split:
            pl.when(jnp.logical_or(follows, c >= ahead))(lambda: south_done(t, c))
        else:
            south_done(t, c)

    for t in range(1, STEPS + 1):
        sides_done(t - 1, 0)
        if t == 1 and split:
            half = (rows - 2) // 6
            over(1, half, 0, columns, functools.partial(march, t))
            let_go()
            over(1 + half, rows - 2 - half, 0, columns, functools.partial(march, t))
        else:
            over(*blocks[0], 0, columns, functools.partial(march, t))
        if t < STEPS:
            sides_start(t, (0,))
        else:
            upwards(lambda hop: total(hop, 0, *blocks[0], 0, columns).start())
            from_below(lambda hop: total(hop, 0, *blocks[0], 0, columns).wait_recv())
            over(*blocks[0], 0, columns, finish)
        sides_done(t - 1, 1)

        def rim(c):
            if t < STEPS:
                take_south(t - 1, c)
                rim_over(c, functools.partial(march, t))
                if t < STEPS - 1:
                    send_chunk(t, c)
                else:
                    send_last(c)
            else:
                pl.when(c == chunks - 1)(keep_last)
                take_south(t - 1, c)

                @pl.when(jnp.logical_or(c < chunks - 1, places["down"] < last_rank))
                def _():
                    rim_over(c, functools.partial(march, t))
                    send_rim_totals(c)

        each(chunks, rim)
        if t == STEPS - 1:
            each(lag, lambda c: south(t, 1 - first, chunks - lag + c).start())
        if t < STEPS:
            sides_start(t, (1, 2))
    keep_south()
    take_rim_totals()
    done(u.at[:, pl.ds(0, 2), pl.ds(depth, cells), :], south_send)
    done(u.at[:, pl.ds(0, rows), pl.ds(0, both), :], side_send)
    upwards(lambda hop: done(totals, tot_send.at[hop - 1]))


def write_out(sizes, depth, pot, end, last_u, last_flows, last_halos, totals_in, pot_out, end_out,
              rim_pot, last_end, sems):
    rows, cells, levels = pot.shape
    columns = cells // depth
    group = group_of(columns)
    width = chunk_of(columns, group)
    base = columns - width
    kept = base * depth
    sides = ((0, 0), (1, rows - 1))

    def write(i, src, dst):
        pltpu.make_async_copy(src, dst, sems.at[i]).start()

    for i, (src, dst) in enumerate(((pot, pot_out), (end, end_out))):
        for y in range(1, rows - 1):
            write(i, src.at[y], dst.at[y])
    if kept:
        for _, y in sides:
            write(1, end.at[y, pl.ds(0, kept)], end_out.at[y, pl.ds(0, kept)])

    def at(x):
        return pl.ds(pl.multiple_of(x * depth, 8), depth)

    def last(i):
        side, x0 = i % 2, pl.multiple_of((i // 2) * group, group)
        flows = [last_flows.at[k] for k in (0, 1, 2)]
        values = new_values(depth, group, last_u, last_halos, *flows, 1, 3 * side, side, x0)
        for g, value in enumerate(values):
            last_end[side, at(x0 + g), :] = value
            x = base + x0 + g
            rim_pot[side, at(x), :] = finished(sizes, totals_in, side * (rows - 1), x, running_sum(value))

    def before(i):
        side, x0 = i % 2, pl.multiple_of((i // 2) * group, group)
        y = side * (rows - 1)
        for g in range(group):
            rim_pot[side, at(x0 + g), :] = finished(sizes, totals_in, y, x0 + g, pot[y, at(x0 + g), :])

    each(2 * (base // group), before)
    each(2 * (width // group), last)
    for side, y in sides:
        write(0, rim_pot.at[side], pot_out.at[y])
        write(1, last_end.at[side], end_out.at[y, pl.ds(kept, cells - kept)])
    pltpu.make_async_copy(pot, pot_out, sems.at[0]).wait()
    pltpu.make_async_copy(end, end_out, sems.at[1]).wait()


def local(sizes, field_values, *flows):
    rows, columns, depth, levels = field_values.shape
    cells = columns * depth
    width = chunk_of(columns, group_of(columns))
    flat = [array.reshape(rows, cells, levels) for array in (field_values, *flows)]
    block = pltpu.VMEM((rows, cells, levels), jnp.float32)
    dma = pltpu.SemaphoreType.DMA
    others = sizes["down"] - 1
    face = (rows, columns, levels)
    out = jax.ShapeDtypeStruct((rows, cells, levels), jnp.float32)
    in_vmem = pl.BlockSpec(memory_space=pltpu.VMEM)
    last = pltpu.VMEM((2, width * depth, levels), jnp.float32)
    held_shapes = (
        block, block,
        pltpu.VMEM((1, 6, (width + 2) * depth, levels), jnp.float32),
        pltpu.VMEM((3, 2, width * depth, levels), jnp.float32),
        pltpu.VMEM((1, 2, 2, width, levels), jnp.float32),
        pltpu.VMEM((others, *face), jnp.float32),
    )
    held = pl.pallas_call(
        functools.partial(kernel, sizes, depth),
        out_shape=held_shapes,
        in_specs=[pl.BlockSpec(memory_space=pl.ANY)] * 4,
        out_specs=(in_vmem,) * len(held_shapes),
        scratch_shapes=[
            pltpu.VMEM((STEPS, rows + 2, cells + 2 * depth, levels), jnp.float32),
            block, block, block,
            pltpu.VMEM((STEPS, 2, *face), jnp.float32),
            pltpu.VMEM((STEPS, 2, *face), jnp.float32),
            pltpu.VMEM(face, jnp.float32),
            dma((2, columns // width)), dma((2, 2)), dma((others, 2)),
            dma, dma, dma((others,)),
            pltpu.SemaphoreType.REGULAR,
        ],
        compiler_params=pltpu.CompilerParams(
            collective_id=0, has_side_effects=True, vmem_limit_bytes=48 * 1024 * 1024),
    )(*flat)
    results = pl.pallas_call(
        functools.partial(write_out, sizes, depth),
        out_shape=(out, out),
        in_specs=[in_vmem] * len(held_shapes),
        out_specs=(pl.BlockSpec(memory_space=pltpu.HBM),) * 2,
        scratch_shapes=[pltpu.VMEM((2, cells, levels), jnp.float32), last, dma((2,))],
        compiler_params=pltpu.CompilerParams(vmem_limit_bytes=8 * 1024 * 1024),
    )(*held)
    return tuple(array.reshape(rows, columns, depth, levels) for array in results)


def solution(mesh):
    spec = P("south", "east", "down", None)
    sizes = {axis: mesh.shape[axis] for axis in AXES}
    return jax.shard_map(
        functools.partial(local, sizes), mesh=mesh, in_specs=(spec,) * 4,
        out_specs=(spec, spec), check_vma=False)
```

```python
import functools

import jax
import jax.numpy as jnp
from jax import lax
from jax.experimental import pallas as pl
from jax.experimental.pallas import tpu as pltpu
from jax.sharding import PartitionSpec as P

STEPS = 4
AXES = ("south", "east", "down")
MESH = pl.DeviceIdType.MESH


def group_of(columns):
    return next(size for size in (8, 4, 2, 1) if columns % size == 0)


def chunk_of(columns, group):
    return next(size for size in (3 * group, 2 * group, group) if columns % size == 0)


def each(count, body):
    def one(i, carry):
        body(i)
        return carry

    lax.fori_loop(0, count, one, 0)


def new_values(depth, group, u, halos, fy, fx, fz, t, y, row, x0):
    levels = u.shape[-1]
    place = lax.broadcasted_iota(jnp.int32, (depth, levels), 0)

    def at(x, pad):
        return pl.ds(pl.multiple_of((x + pad) * depth, 8), depth)

    line = [u[t - 1, y + 1, at(x0 + g, 0), :] for g in range(group + 2)]
    values = []
    for g in range(group):
        x = x0 + g
        mid, west, east_of = line[g + 1], line[g], line[g + 2]
        north, south_of = u[t - 1, y, at(x, 1), :], u[t - 1, y + 2, at(x, 1), :]
        low = jnp.broadcast_to(halos[t - 1, 0, row, pl.ds(x, 1), :], (depth, levels))
        high = jnp.broadcast_to(halos[t - 1, 1, row, pl.ds(x, 1), :], (depth, levels))
        low = jnp.where(place == 0, low, pltpu.roll(mid, 1, 0))
        high = jnp.where(place == depth - 1, high, pltpu.roll(mid, depth - 1, 0))
        own = at(x, 0)
        spread = (north + south_of) + (west + east_of) + (low + high) - 6.0 * mid
        values.append(mid - fy[row, own, :] * (south_of - north) - fx[row, own, :] * (east_of - west)
                      - fz[row, own, :] * (high - low) + 0.05 * spread)
    return values


def running_sum(value):
    depth = value.shape[0]
    place = lax.broadcasted_iota(jnp.int32, value.shape, 0)
    hop = 1
    while hop < depth:
        value = value + jnp.where(place >= hop, pltpu.roll(value, hop, 0), 0.0)
        hop *= 2
    return value


def finished(sizes, totals_in, row, x, value):
    rank = lax.axis_index("down")
    for hop in range(1, sizes["down"]):
        below = jnp.broadcast_to(totals_in[hop - 1, row, pl.ds(x, 1), :], value.shape)
        value = value + jnp.where(rank >= hop, below, 0.0)
    return value * (1.0 / (value.shape[0] * sizes["down"]))


def kernel(sizes, depth, field, flow_y, flow_x, flow_z, pot, end, last_u, last_flows, last_halos, totals_in,
           u, fy, fx, fz, faces, halos, totals, south_recv, side_recv, tot_recv, south_send, side_send, tot_send, go):
    rows, cells, levels = field.shape
    columns = cells // depth
    group = group_of(columns)
    width = chunk_of(columns, group)
    chunks = columns // width
    places = {axis: lax.axis_index(axis) for axis in AXES}

    def beside(axis, hop):
        return {axis: lax.rem(places[axis] + hop, sizes[axis])}

    near = lax.rem(places["south"], 2)
    leads = lax.rem(places["down"], 2) == 0
    follows = jnp.logical_not(leads)
    split = sizes["down"] == 2 and sizes["south"] % 2 == 0 and sizes["south"] > 2
    hops = [(axis, hop) for axis in ("south", "east") for hop in sorted({1, sizes[axis] - 1})]
    barrier = pltpu.get_barrier_semaphore()
    partner = beside("south", 1 + near * (sizes["south"] - 2))

    def greet(device_id):
        pl.semaphore_signal(barrier, inc=1, device_id=device_id, device_id_type=MESH)

    if split:
        @pl.when(follows)
        def _():
            greet(partner)
            greet({"down": 0})

        for axis, hop in hops:
            greet({**beside(axis, hop), "down": 0})
    else:
        hops += [("down", hop) for hop in range(1, sizes["down"])]
        for axis, hop in hops:
            greet(beside(axis, hop))

    def load(src, dst, sem):
        return pltpu.make_async_copy(src, dst, sem)

    def done(ref, sem):
        pltpu.make_async_copy(ref, ref, sem).wait()

    rims_sem, inner_sem, flows_sem = side_recv.at[1, 0], side_recv.at[1, 1], tot_recv.at[0, 0]
    rims = [load(field.at[y], u.at[0, y + 1, pl.ds(depth, cells), :], rims_sem) for y in (0, rows - 1)]
    inner = load(field.at[pl.ds(1, rows - 2)], u.at[0, pl.ds(2, rows - 2), pl.ds(depth, cells), :], inner_sem)
    flows = [load(src, dst, flows_sem) for src, dst in ((flow_y, fy), (flow_x, fx), (flow_z, fz))]
    for copy in rims:
        copy.start()

    def chunk_at(c):
        return pl.ds(pl.multiple_of(c * width * depth + depth, 8), width * depth)

    def south(t, side, c):
        return pltpu.make_async_remote_copy(
            src_ref=u.at[t, (1 - side) * (rows - 1) + 1, chunk_at(c), :],
            dst_ref=u.at[t, side * (rows + 1), chunk_at(c), :],
            send_sem=south_send, recv_sem=south_recv.at[t % 2, c],
            device_id=beside("south", 1 + side * (sizes["south"] - 2)), device_id_type=MESH)

    def south_done(t, c):
        done(u.at[t, pl.ds(0, 2), chunk_at(c), :], south_recv.at[t % 2, c])

    blocks = ((1, rows - 2), (0, 1), (rows - 1, 1))

    def east(t, side, part):
        start, count = blocks[part]
        column = columns if side == 0 else 1
        if t == 0:
            src = field.at[pl.ds(start, count), pl.ds((column - 1) * depth, depth), :]
        else:
            src = u.at[t, pl.ds(start + 1, count), pl.ds(column * depth, depth), :]
        return pltpu.make_async_remote_copy(
            src_ref=src,
            dst_ref=u.at[t, pl.ds(start + 1, count), pl.ds(0 if side == 0 else cells + depth, depth), :],
            send_sem=side_send, recv_sem=side_recv.at[t % 2, min(part, 1)],
            device_id=beside("east", 1 if side == 0 else sizes["east"] - 1), device_id_type=MESH)

    def down(t, side, part):
        start, count = blocks[part]
        return pltpu.make_async_remote_copy(
            src_ref=faces.at[t, side, pl.ds(start, count)],
            dst_ref=halos.at[t, side, pl.ds(start, count)],
            send_sem=side_send, recv_sem=side_recv.at[t % 2, min(part, 1)],
            device_id=beside("down", 1 if side == 0 else sizes["down"] - 1), device_id_type=MESH)

    def sides_start(t, parts):
        for part in parts:
            for side in (0, 1):
                down(t, side, part).start()
                east(t, side, part).start()

    both = 2 * (depth + columns)

    def sides_done(t, part):
        done(u.at[t, pl.ds(0, rows - 2 if part == 0 else 2), pl.ds(0, both), :], side_recv.at[t % 2, part])

    def total(hop, piece, y0, count, x0, span):
        cut = (pl.ds(y0, count), pl.ds(x0, span))
        return pltpu.make_async_remote_copy(
            src_ref=totals.at[cut], dst_ref=totals_in.at[(hop - 1, *cut)],
            send_sem=tot_send.at[hop - 1], recv_sem=tot_recv.at[hop - 1, piece],
            device_id=beside("down", hop), device_id_type=MESH)

    def rim_at(c):
        return pl.multiple_of(c * width, group)

    def take_faces(t, y, x0):
        for side, place in ((0, depth - 1), (1, 0)):
            start = (x0 + 1) * depth + place
            faces[t, side, y, pl.ds(x0, group), :] = u[t, y + 1, pl.ds(start, group, stride=depth), :]

    def march(t, y, x0):
        values = new_values(depth, group, u, halos, fy, fx, fz, t, y, y, x0)
        for g, value in enumerate(values):
            if t < STEPS:
                u[t, y + 1, pl.ds(pl.multiple_of((x0 + g + 1) * depth, 8), depth), :] = value
            else:
                own = pl.ds(pl.multiple_of((x0 + g) * depth, 8), depth)
                end[y, own, :] = value
                pot[y, own, :] = running_sum(value)
        if t < STEPS:
            take_faces(t, y, x0)
        else:
            start = x0 * depth + depth - 1
            totals[y, pl.ds(x0, group), :] = pot[y, pl.ds(start, group, stride=depth), :]

    def over(y0, count, x0, span, body):
        groups = span // group
        each(count * groups,
             lambda i: body(y0 + i // groups, pl.multiple_of(x0 + (i % groups) * group, group)))

    def finish(y, x0):
        for g in range(group):
            own = pl.ds(pl.multiple_of((x0 + g) * depth, 8), depth)
            pot[y, own, :] = finished(sizes, totals_in, y, x0 + g, pot[y, own, :])

    down_hops = range(1, sizes["down"])
    last_rank = sizes["down"] - 1

    def upwards(body):
        for hop in down_hops:
            pl.when(places["down"] + hop <= last_rank)(functools.partial(body, hop))

    def from_below(body):
        for hop in down_hops:
            pl.when(places["down"] >= hop)(functools.partial(body, hop))

    def rim_over(c, body):
        groups = width // group
        each(2 * groups, lambda i: body((i // groups) * (rows - 1),
                                        pl.multiple_of(c * width + (i % groups) * group, group)))

    last_block = sizes["south"] - 1
    first = jnp.where(places["south"] == last_block, 0, jnp.where(places["south"] == 1, 1, 1 - near))
    lag = min(3, chunks)

    def send_chunk(t, c):
        south(t, 1 - near, c).start()
        south(t, near, c).start()

    def send_last(c):
        south(STEPS - 1, first, c).start()
        pl.when(c >= lag)(lambda: south(STEPS - 1, 1 - first, c - lag).start())

    def send_first():
        each(chunks, lambda c: send_chunk(0, c))

    def send_far():
        each(chunks, lambda c: south(0, 1 - near, c).start())

    def send_rim_totals(c):
        def one(hop):
            for y in (0, rows - 1):
                total(hop, 1, y, 1, rim_at(c), width).start()

        upwards(one)

    def take_rim_totals():
        from_below(lambda hop: done(totals_in.at[hop - 1, pl.ds(0, 2)], tot_recv.at[hop - 1, 1]))

    base = columns - width
    last_cells = pl.ds(base * depth, width * depth)

    def keep_last():
        for side in (0, 1):
            row = side * (rows - 1)
            for i in (0, 1, 2):
                if (side, i) not in ((0, 0), (1, 2)):
                    last_u[0, 3 * side + i] = u[STEPS - 1, row + i, pl.ds(base * depth, (width + 2) * depth), :]
            for i, flow in enumerate((fy, fx, fz)):
                last_flows[i, side] = flow[row, last_cells, :]
            for z in (0, 1):
                last_halos[0, z, side] = halos[STEPS - 1, z, row, pl.ds(base, width), :]

    def keep_south():
        for side in (0, 1):
            last_u[0, 5 * side, pl.ds(depth, width * depth), :] = u[
                STEPS - 1, side * (rows + 1), pl.ds((base + 1) * depth, width * depth), :]

    if split:
        @pl.when(jnp.logical_and(follows, near == 1))
        def _():
            pl.semaphore_wait(barrier, 1)
            pltpu.make_async_remote_copy(
                src_ref=field.at[(1 - near) * (rows - 1), pl.ds(0, width * depth), :],
                dst_ref=u.at[0, near * (rows + 1), pl.ds(depth, width * depth), :],
                send_sem=south_send, recv_sem=south_recv.at[0, 0], device_id=partner, device_id_type=MESH).start()
    else:
        pl.semaphore_wait(barrier, len(hops))
    done(u.at[0, pl.ds(1, 2), pl.ds(depth, cells), :], rims_sem)
    inner.start()
    for copy in flows:
        copy.start()
    if split:
        @pl.when(leads)
        def _():
            pl.semaphore_wait(barrier, 2 * len(hops) + 1)
            pl.semaphore_signal(go, inc=1, device_id={"down": 1}, device_id_type=MESH)

        @pl.when(jnp.logical_and(follows, near == 0))
        def _():
            pl.semaphore_wait(barrier, 1)
            south(0, near, 0).start()

        @pl.when(follows)
        def _():
            each(chunks - 1, lambda c: south(0, near, c + 1).start())
    pl.when(leads)(send_first)
    done(u.at[0, pl.ds(2, rows - 2), pl.ds(depth, cells), :], inner_sem)
    over(0, rows, 0, columns, functools.partial(take_faces, 0))
    if split:
        pl.when(follows)(lambda: pl.semaphore_wait(go, 1))
    sides_start(0, (0, 1, 2))
    if not split:
        pl.when(follows)(send_first)
    done(u.at[pl.ds(0, 3), pl.ds(0, rows), pl.ds(depth, cells), :], flows_sem)

    ahead = min(2, chunks) if split else 0

    def let_go():
        @pl.when(leads)
        def _():
            each(ahead, lambda c: south_done(0, c))
            pl.semaphore_signal(go, inc=1, device_id={"down": 1}, device_id_type=MESH)

        @pl.when(follows)
        def _():
            pl.semaphore_wait(go, 1)
            send_far()

    def take_south(t, c):
        if t == 0 and split:
            pl.when(jnp.logical_or(follows, c >= ahead))(lambda: south_done(t, c))
        else:
            south_done(t, c)

    for t in range(1, STEPS + 1):
        sides_done(t - 1, 0)
        if t == 1 and split:
            half = (rows - 2) // 6
            over(1, half, 0, columns, functools.partial(march, t))
            let_go()
            over(1 + half, rows - 2 - half, 0, columns, functools.partial(march, t))
        else:
            over(*blocks[0], 0, columns, functools.partial(march, t))
        if t < STEPS:
            sides_start(t, (0,))
        else:
            upwards(lambda hop: total(hop, 0, *blocks[0], 0, columns).start())
            from_below(lambda hop: total(hop, 0, *blocks[0], 0, columns).wait_recv())
            over(*blocks[0], 0, columns, finish)
        sides_done(t - 1, 1)

        def rim(c):
            if t < STEPS:
                take_south(t - 1, c)
                rim_over(c, functools.partial(march, t))
                if t < STEPS - 1:
                    send_chunk(t, c)
                else:
                    send_last(c)
            else:
                pl.when(c == chunks - 1)(keep_last)
                take_south(t - 1, c)

                @pl.when(jnp.logical_or(c < chunks - 1, places["down"] < last_rank))
                def _():
                    rim_over(c, functools.partial(march, t))
                    send_rim_totals(c)

        each(chunks, rim)
        if t == STEPS - 1:
            each(lag, lambda c: south(t, 1 - first, chunks - lag + c).start())
        if t < STEPS:
            sides_start(t, (1, 2))
    keep_south()
    take_rim_totals()
    done(u.at[:, pl.ds(0, 2), pl.ds(depth, cells), :], south_send)
    done(u.at[:, pl.ds(0, rows), pl.ds(0, both), :], side_send)
    upwards(lambda hop: done(totals, tot_send.at[hop - 1]))


def write_out(sizes, depth, pot, end, last_u, last_flows, last_halos, totals_in, pot_out, end_out,
              rim_pot, last_end, sems):
    rows, cells, levels = pot.shape
    columns = cells // depth
    group = group_of(columns)
    width = chunk_of(columns, group)
    base = columns - width
    kept = base * depth
    sides = ((0, 0), (1, rows - 1))

    def write(i, src, dst):
        pltpu.make_async_copy(src, dst, sems.at[i]).start()

    for i, (src, dst) in enumerate(((pot, pot_out), (end, end_out))):
        for y in range(1, rows - 1):
            write(i, src.at[y], dst.at[y])
    if kept:
        for _, y in sides:
            write(1, end.at[y, pl.ds(0, kept)], end_out.at[y, pl.ds(0, kept)])

    def at(x):
        return pl.ds(pl.multiple_of(x * depth, 8), depth)

    def last(i):
        side, x0 = i % 2, pl.multiple_of((i // 2) * group, group)
        flows = [last_flows.at[k] for k in (0, 1, 2)]
        values = new_values(depth, group, last_u, last_halos, *flows, 1, 3 * side, side, x0)
        for g, value in enumerate(values):
            last_end[side, at(x0 + g), :] = value
            x = base + x0 + g
            rim_pot[side, at(x), :] = finished(sizes, totals_in, side * (rows - 1), x, running_sum(value))

    def before(i):
        side, x0 = i % 2, pl.multiple_of((i // 2) * group, group)
        y = side * (rows - 1)
        for g in range(group):
            rim_pot[side, at(x0 + g), :] = finished(sizes, totals_in, y, x0 + g, pot[y, at(x0 + g), :])

    each(2 * (base // group), before)
    each(2 * (width // group), last)
    for side, y in sides:
        write(0, rim_pot.at[side], pot_out.at[y])
        write(1, last_end.at[side], end_out.at[y, pl.ds(kept, cells - kept)])
    pltpu.make_async_copy(pot, pot_out, sems.at[0]).wait()
    pltpu.make_async_copy(end, end_out, sems.at[1]).wait()


def local(sizes, field_values, *flows):
    rows, columns, depth, levels = field_values.shape
    cells = columns * depth
    width = chunk_of(columns, group_of(columns))
    flat = [array.reshape(rows, cells, levels) for array in (field_values, *flows)]
    block = pltpu.VMEM((rows, cells, levels), jnp.float32)
    dma = pltpu.SemaphoreType.DMA
    others = sizes["down"] - 1
    face = (rows, columns, levels)
    out = jax.ShapeDtypeStruct((rows, cells, levels), jnp.float32)
    in_vmem = pl.BlockSpec(memory_space=pltpu.VMEM)
    last = pltpu.VMEM((2, width * depth, levels), jnp.float32)
    held_shapes = (
        block, block,
        pltpu.VMEM((1, 6, (width + 2) * depth, levels), jnp.float32),
        pltpu.VMEM((3, 2, width * depth, levels), jnp.float32),
        pltpu.VMEM((1, 2, 2, width, levels), jnp.float32),
        pltpu.VMEM((others, *face), jnp.float32),
    )
    held = pl.pallas_call(
        functools.partial(kernel, sizes, depth),
        out_shape=held_shapes,
        in_specs=[pl.BlockSpec(memory_space=pl.ANY)] * 4,
        out_specs=(in_vmem,) * len(held_shapes),
        scratch_shapes=[
            pltpu.VMEM((STEPS, rows + 2, cells + 2 * depth, levels), jnp.float32),
            block, block, block,
            pltpu.VMEM((STEPS, 2, *face), jnp.float32),
            pltpu.VMEM((STEPS, 2, *face), jnp.float32),
            pltpu.VMEM(face, jnp.float32),
            dma((2, columns // width)), dma((2, 2)), dma((others, 2)),
            dma, dma, dma((others,)),
            pltpu.SemaphoreType.REGULAR,
        ],
        compiler_params=pltpu.CompilerParams(
            collective_id=0, has_side_effects=True, vmem_limit_bytes=48 * 1024 * 1024),
    )(*flat)
    results = pl.pallas_call(
        functools.partial(write_out, sizes, depth),
        out_shape=(out, out),
        in_specs=[in_vmem] * len(held_shapes),
        out_specs=(pl.BlockSpec(memory_space=pltpu.HBM),) * 2,
        scratch_shapes=[pltpu.VMEM((2, cells, levels), jnp.float32), last, dma((2,))],
        compiler_params=pltpu.CompilerParams(vmem_limit_bytes=8 * 1024 * 1024),
    )(*held)
    return tuple(array.reshape(rows, columns, depth, levels) for array in results)


def solution(mesh):
    spec = P("south", "east", "down", None)
    sizes = {axis: mesh.shape[axis] for axis in AXES}
    return jax.shard_map(
        functools.partial(local, sizes), mesh=mesh, in_specs=(spec,) * 4,
        out_specs=(spec, spec), check_vma=False)
```
